8 devices in a mesh: dp: 1 (over z), tp: 8 (over x, y, core).
Axes of the slice: x: 2, y: 2, z: 1, core: 2. Of those that a mesh axis runs over, the one named last changes fastest.
Arguments:
- x: bfloat16 [2048, 4096], P(('dp', 'tp'))
- w_gate: bfloat16 [4096, 14336], P(None, 'tp')
- w_up: bfloat16 [4096, 14336], P(None, 'tp')
- w_down: bfloat16 [14336, 4096], P('tp')
Outputs:
- output: bfloat16 [2048, 4096], P(('dp', 'tp'))
All inputs are finite; a program needn't handle non-finite values.
Results may differ from the reference program's by a relative error of at most 0.016.
Values are sent between devices in bfloat16 or wider.
A program may use at most 2 GiB of HBM per device.

```python
import jax
import jax.numpy as jnp

ROWS = 2048
D = 4096
FF = 14336


def setup_inputs(seed: int = 0, part: int = 0) -> dict:
    kx, kg, ku, kd = jax.random.split(jax.random.key(seed), 4)
    drawn = {
        "x": jax.random.normal(jax.random.fold_in(kx, part), (ROWS, D), jnp.float32),
        "w_gate": jax.random.normal(kg, (D, FF), jnp.float32) * D**-0.5,
        "w_up": jax.random.normal(ku, (D, FF), jnp.float32) * D**-0.5,
        "w_down": jax.random.normal(kd, (FF, D), jnp.float32) * FF**-0.5,
    }
    return {k: v.astype(jnp.bfloat16) for k, v in drawn.items()}


def reference(x, w_gate, w_up, w_down):
    gate = jnp.dot(x, w_gate, preferred_element_type=jnp.float32)
    up = jnp.dot(x, w_up, preferred_element_type=jnp.float32)
    hidden = (jax.nn.silu(gate) * up).astype(jnp.bfloat16)
    return jnp.dot(hidden, w_down, preferred_element_type=jnp.float32).astype(jnp.bfloat16)
```

```python
import jax
import jax.numpy as jnp
from jax import lax
from jax.sharding import PartitionSpec as P


F32 = jnp.float32
BF16 = jnp.bfloat16


def solution(mesh):
    n = mesh.shape["tp"]

    def send(a, mask):
        return lax.ppermute(a, "tp", [(i, i ^ mask) for i in range(n)])

    def step(x, w_gate, w_up, w_down):
        half = x.shape[0] // 2
        rows = x.shape[0]

        def mlp(a):
            gate = jnp.dot(a, w_gate, preferred_element_type=F32)
            up = jnp.dot(a, w_up, preferred_element_type=F32)
            hidden = (jax.nn.silu(gate) * up).astype(BF16)
            return jnp.dot(hidden, w_down, preferred_element_type=F32)

        def block(a, b):
            term = mlp(jnp.concatenate([a, b], axis=0))
            return term[:rows] + send(term[rows:].astype(BF16), 1).astype(F32)

        from_x = send(x, 4)
        from_y = send(x, 2)
        diag = jnp.concatenate([send(from_x[:half], 2), send(from_y[half:], 4)], axis=0)
        sum_x = block(from_x, send(from_x, 1))
        sum_d = block(diag, send(diag, 1))
        sum_y = block(from_y, send(from_y, 1))
        own = block(x, send(x, 1))
        via_x = send(sum_d[:half].astype(BF16), 4)
        via_y = send(sum_d[half:].astype(BF16), 2)
        out_y = jnp.concatenate([sum_y[:half] + via_x.astype(F32), sum_y[half:]], axis=0)
        out_x = jnp.concatenate([sum_x[:half], sum_x[half:] + via_y.astype(F32)], axis=0)
        got_x = send(out_x.astype(BF16), 4)
        got_y = send(out_y.astype(BF16), 2)
        return (own + got_x.astype(F32) + got_y.astype(F32)).astype(BF16)

    return jax.shard_map(
        step,
        mesh=mesh,
        in_specs=(P(("dp", "tp"), None), P(None, "tp"), P(None, "tp"), P("tp", None)),
        out_specs=P(("dp", "tp"), None),
        check_vma=False,
    )
```

```python
import jax
import jax.numpy as jnp
from jax import lax
from jax.experimental import pallas as pl
from jax.experimental.pallas import tpu as pltpu
from jax.sharding import PartitionSpec as P

F32 = jnp.float32
BF16 = jnp.bfloat16
MESH = pl.DeviceIdType.MESH

SIB, YN, XN = 1, 2, 4
LINK = (XN, YN)
OWN, FX, FY, DG = 0, 1, 2, 3
PIECE = 64
STEPS = 8
GT = 256
DT = 1024


def body(
    x, wg_h, wu_h, wd_h, y, xg, fh,
    wg, wu, wd, xb, hb, mine, tsend, trecv, outd, outg, rly, hold, fv,
    so, ro, sr, rr, ss, rs, st, rt, sd, rd, sg, rg, sq, rq, lx, lw, lf, ly,
):
    me = lax.axis_index("tp")
    d = x.shape[1]
    half = d // 2
    ff = wg.shape[1]
    cols = (pl.ds(0, half), pl.ds(half, half))

    def remote(src, dst, send, recv, mask):
        return pltpu.make_async_remote_copy(
            src_ref=src, dst_ref=dst, send_sem=send, recv_sem=recv,
            device_id={"tp": me ^ mask}, device_id_type=MESH,
        )

    def rows(k, n=1):
        return pl.ds(k * PIECE, n * PIECE)

    def own(l, k):
        return remote(x.at[rows(k)], xg.at[FX + l, 0, rows(k)], so.at[l, k], ro.at[l, k], LINK[l])

    def relay(l, r):
        src = xg.at[FY - l, 0, rows(2 * r + l)]
        return remote(src, xg.at[DG, 0, rows(2 * r + l)], sr.at[l, r], rr.at[l, r], LINK[l])

    def hand(b, k):
        if b == OWN:
            return remote(x, xg.at[OWN, 1], ss.at[0, 0], rs.at[0, 0], SIB)
        return remote(xg.at[b, 0, rows(k)], xg.at[b, 1, rows(k)], ss.at[b, k], rs.at[b, k], SIB)

    def term(s):
        slot = s % 2
        return remote(tsend, trecv.at[slot], st.at[slot], rt.at[slot], SIB)

    def landing(l, k):
        return fh.at[l, k] if k < 2 else fv.at[l, k - 2]

    def direct(l, k):
        return remote(
            outd.at[k, rows(l)], landing(l, k).at[:, cols[l]], sd.at[l, k], rd.at[l, k], LINK[l]
        )

    def diag(l, c):
        return remote(outg.at[c, :, cols[l]], rly.at[c, l], sg.at[l, c], rg.at[l, c], LINK[l])

    def relayed(l, k):
        src = rly.at[k // 2, 1 - l, rows(k % 2)]
        return remote(src, landing(l, k).at[:, cols[1 - l]], sq.at[l, k], rq.at[l, k], LINK[l])

    def pieces(s):
        if s < 4:
            return ((FX, s), (FY, s))
        b, c = (DG, s - 4) if s < 6 else (OWN, s - 6)
        return ((b, 2 * c), (b, 2 * c + 1))

    def load(s, side):
        out = []
        for i, (b, k) in enumerate(pieces(s)):
            src = x.at[rows(k)] if (b == OWN and side == 0) else xg.at[b, side, rows(k)]
            out.append(pltpu.make_async_copy(src, xb.at[rows(2 * side + i)], lx.at[side, i]))
        return out

    def take(s):
        if s < 4:
            for l in range(2):
                own(l, s).wait_recv()
        elif s < 6:
            for l in range(2):
                relay(l, s - 4).wait_recv()
        if s < 6:
            for b, k in pieces(s):
                hand(b, k).start()
        for c in load(s, 0):
            c.start()
        if s == 1:
            for l in range(2):
                relay(l, 0).start()
        if s == 3:
            for l in range(2):
                relay(l, 1).start()

    def take_other(s):
        if s < 6:
            for b, k in pieces(s):
                hand(b, k).wait_recv()
        elif s == 6:
            hand(OWN, 0).wait_recv()
        for c in load(s, 1):
            c.start()

    weights = [
        pltpu.make_async_copy(h, v, lw.at[i])
        for i, (h, v) in enumerate(((wg_h, wg), (wu_h, wu), (wd_h, wd)))
    ]

    def total(r, slot):
        return mine[r] + trecv[slot, r].astype(F32)

    def blocks(n, f):
        def one(i, carry):
            f(pl.multiple_of(i * 16, 16))
            return carry

        lax.fori_loop(0, n, one, 0)

    def settle(p):
        slot = p % 2
        term(p).wait_recv()
        if p < 4:
            for l in range(2):

                def f(i, l=l):
                    r = pl.ds(l * PIECE + i, 16)
                    v = total(r, slot)
                    a, b = v[:, :half], v[:, half:]
                    outd[p, r] = (b if l else a).astype(BF16)
                    hold[p, r] = a if l else b

                blocks(PIECE // 16, f)
                direct(l, p).start()
        elif p < 6:

            def f(i):
                r = pl.ds(i, 16)
                outg[p - 4, r] = total(r, slot).astype(BF16)

            blocks(8, f)
            for l in range(2):
                diag(l, p - 4).start()
        else:

            def f(i):
                r = pl.ds(i, 16)
                v = total(r, slot)
                hold[0, r] = v[:, :half]
                hold[1, r] = v[:, half:]

            blocks(8, f)

    def pass_on(c):
        for l in range(2):
            diag(1 - l, c).wait_recv()
        for k in (2 * c, 2 * c + 1):
            for l in range(2):

                def f(i, k=k, l=l):
                    r = pl.ds((k % 2) * PIECE + i, 16)
                    v = hold[k, pl.ds(l * PIECE + i, 16)] + rly[c, 1 - l, r].astype(F32)
                    rly[c, 1 - l, r] = v.astype(BF16)

                blocks(PIECE // 16, f)
                relayed(l, k).start()

    def gate_up(lo, hi):
        def one(j, carry):
            c = pl.ds(pl.multiple_of(j * GT, GT), GT)
            g = jnp.dot(xb[...], wg[:, c], preferred_element_type=F32)
            u = jnp.dot(xb[...], wu[:, c], preferred_element_type=F32)
            hb[:, c] = (jax.nn.silu(g) * u).astype(BF16)
            return carry

        lax.fori_loop(lo, hi, one, 0)

    def down(lo, hi):
        def one(j, carry):
            c = pl.ds(pl.multiple_of(j * DT, DT), DT)
            t = jnp.dot(hb[...], wd[:, c], preferred_element_type=F32)
            mine[:, c] = t[: 2 * PIECE]
            tsend[:, c] = t[2 * PIECE :].astype(BF16)
            return carry

        lax.fori_loop(lo, hi, one, 0)

    barrier = pltpu.get_barrier_semaphore()
    for mask in (SIB, YN, XN):
        pl.semaphore_signal(barrier, inc=1, device_id={"tp": me ^ mask}, device_id_type=MESH)
    pl.semaphore_wait(barrier, 3)

    for k in range(4):
        for l in range(2):
            own(l, k).start()
    for w in weights:
        w.start()
    take(0)
    take_other(0)
    hand(OWN, 0).start()
    weights[0].wait()
    weights[1].wait()

    def at(s, table):
        for k, fs in table.items():

            @pl.when(s == k)
            def _(fs=fs):
                for f, *args in fs:
                    f(*args)

    after_tiles = {p + 1: [(settle, p)] for p in range(7)}
    after_gate = {s: [(take, s + 1)] for s in range(7)}
    after_gate[0].append((weights[2].wait,))
    after_gate[6].append((pass_on, 0))
    after_gate[7] = [(pass_on, 1)]
    for s in range(1, STEPS):
        after_gate[s].append((term(s - 1).wait_send,))
    late = {s: [(take_other, s + 1)] for s in range(7)}
    ends = {s: [(term(s).start,)] for s in range(STEPS)}

    def step(s, carry):
        for side in range(2):
            for c in load(0, side):
                c.wait()
        gate_up(0, 3)
        at(s, after_tiles)
        gate_up(3, ff // GT)
        at(s, after_gate)
        down(0, d // DT - 1)
        at(s, late)
        down(d // DT - 1, d // DT)
        at(s, ends)
        return carry

    lax.fori_loop(0, STEPS, step, 0)

    for k in range(2):
        for l in range(2):
            direct(l, k).wait_recv()
            relayed(l, k).wait_recv()
    back = [
        pltpu.make_async_copy(fh.at[l, k], xb.at[rows(2 * l + k)], lf.at[l, k])
        for l in range(2)
        for k in range(2)
    ]
    for c in back:
        c.start()
    term(7).wait_recv()
    for k in range(4):
        for l in range(2):
            direct(l, k).wait_send()
    for c in back:
        c.wait()

    def first(i):
        r = pl.ds(i, 16)
        v = xb[r].astype(F32) + xb[pl.ds(128 + i, 16)].astype(F32)
        outd[0, r] = (hold[0, r] + v[:, :half]).astype(BF16)
        outd[1, r] = (hold[1, r] + v[:, half:]).astype(BF16)

    blocks(8, first)
    outs = [
        pltpu.make_async_copy(outd.at[h], y.at[rows(0, 2), cols[h]], ly.at[0, h]) for h in range(2)
    ]
    for c in outs:
        c.start()
    for k in (2, 3):
        for l in range(2):
            direct(l, k).wait_recv()
            relayed(l, k).wait_recv()

        def last(i, k=k):
            r = pl.ds((k - 2) * PIECE + i, 16)
            q = pl.ds(i, 16)
            v = total(r, 1) + fv[0, k - 2, q].astype(F32) + fv[1, k - 2, q].astype(F32)
            outd[2, r] = v[:, :half].astype(BF16)
            outd[3, r] = v[:, half:].astype(BF16)

        blocks(PIECE // 16, last)
        for h in range(2):
            c = pltpu.make_async_copy(
                outd.at[2 + h, rows(k - 2)], y.at[rows(k), cols[h]], ly.at[k - 1, h]
            )
            c.start()
            outs.append(c)
    for c in outs:
        c.wait()
    term(7).wait_send()
    hand(OWN, 0).wait_send()
    for l in range(2):
        for k in range(4):
            own(l, k).wait_send()
            relayed(l, k).wait_send()
        for r in range(2):
            relay(l, r).wait_send()
            diag(l, r).wait_send()
    for b in (FX, FY, DG):
        for k in range(4):
            hand(b, k).wait_send()


def solution(mesh):
    def step(x, w_gate, w_up, w_down):
        r, d = x.shape
        ff = w_gate.shape[1]
        hbm = pl.BlockSpec(memory_space=pl.ANY)
        dma = pltpu.SemaphoreType.DMA
        half = d // 2
        y, _, _ = pl.pallas_call(
            body,
            out_shape=(
                jax.ShapeDtypeStruct((r, d), BF16),
                jax.ShapeDtypeStruct((4, 2, r, d), BF16),
                jax.ShapeDtypeStruct((2, 2, PIECE, d), BF16),
            ),
            in_specs=[hbm] * 4,
            out_specs=(hbm,) * 3,
            scratch_shapes=[
                pltpu.VMEM((d, ff), BF16),
                pltpu.VMEM((d, ff), BF16),
                pltpu.VMEM((ff, d), BF16),
                pltpu.VMEM((256, d), BF16),
                pltpu.VMEM((256, ff), BF16),
                pltpu.VMEM((128, d), F32),
                pltpu.VMEM((128, d), BF16),
                pltpu.VMEM((2, 128, d), BF16),
                pltpu.VMEM((4, 128, half), BF16),
                pltpu.VMEM((2, 128, d), BF16),
                pltpu.VMEM((2, 2, 128, half), BF16),
                pltpu.VMEM((4, 128, half), F32),
                pltpu.VMEM((2, 2, PIECE, d), BF16),
                dma((2, 4)), dma((2, 4)), dma((2, 2)), dma((2, 2)), dma((4, 4)), dma((4, 4)),
                dma((2,)), dma((2,)), dma((2, 4)), dma((2, 4)), dma((2, 2)), dma((2, 2)),
                dma((2, 4)), dma((2, 4)), dma((2, 2)), dma((3,)), dma((2, 2)), dma((3, 2)),
            ],
            compiler_params=pltpu.CompilerParams(
                collective_id=0, has_side_effects=True, vmem_limit_bytes=67043328
            ),
            cost_estimate=pl.CostEstimate(
                flops=6 * 8 * r * d * ff, bytes_accessed=6 * d * ff + 4 * r * d, transcendentals=8 * r * ff
            ),
            name="mlp",
        )(x, w_gate, w_up, w_down)
        return y

    return jax.shard_map(
        step,
        mesh=mesh,
        in_specs=(P(("dp", "tp"), None), P(None, "tp"), P(None, "tp"), P("tp", None)),
        out_specs=P(("dp", "tp"), None),
        check_vma=False,
    )
```

```python
import jax
import jax.numpy as jnp
from jax import lax
from jax.experimental import pallas as pl
from jax.experimental.pallas import tpu as pltpu
from jax.sharding import PartitionSpec as P

F32 = jnp.float32
BF16 = jnp.bfloat16
MESH = pl.DeviceIdType.MESH

SIB, YN, XN = 1, 2, 4
LINK = (XN, YN)
OWN, FX, FY, DG = 0, 1, 2, 3
PIECE = 64
STEPS = 8
X_STEPS = {0: 0, 1: 1, 2: 2, 5: 3}
D_STEPS = {3: 0, 4: 1}
SWAP = (1, 0, 3, 2)
GT = 256
DT = 1024


def body(
    x, wg_h, wu_h, wd_h, y, xg, fh,
    wg, wu, wd, xb, hb, mine, tsend, trecv, outd, outg, rly, hold, fv,
    so, ro, sr, rr, ss, rs, st, rt, sd, rd, sg, rg, sq, rq, lx, lw, lf, ly,
):
    me = lax.axis_index("tp")
    d = x.shape[1]
    half = d // 2
    ff = wg.shape[1]
    cols = (pl.ds(0, half), pl.ds(half, half))

    def remote(src, dst, send, recv, mask):
        return pltpu.make_async_remote_copy(
            src_ref=src, dst_ref=dst, send_sem=send, recv_sem=recv,
            device_id={"tp": me ^ mask}, device_id_type=MESH,
        )

    def rows(k, n=1):
        return pl.ds(k * PIECE, n * PIECE)

    def turn(l, k):
        return SWAP[k] if l else k

    def own(l, k):
        return remote(x.at[rows(k)], xg.at[FX + l, 0, rows(k)], so.at[l, k], ro.at[l, k], LINK[l])

    def relay(l, r):
        k = 2 * r + 1 - l
        return remote(
            xg.at[FY - l, 0, rows(k)], xg.at[DG, 0, rows(k)], sr.at[l, r], rr.at[l, r], LINK[l]
        )

    def hand(b, k):
        if b == OWN:
            return remote(x, xg.at[OWN, 1], ss.at[0, 0], rs.at[0, 0], SIB)
        return remote(xg.at[b, 0, rows(k)], xg.at[b, 1, rows(k)], ss.at[b, k], rs.at[b, k], SIB)

    def term(s):
        slot = s % 2
        return remote(tsend, trecv.at[slot], st.at[slot], rt.at[slot], SIB)

    def landing(l, k):
        return fh.at[l, k] if k < 2 else fv.at[l, k - 2]

    def direct(l, k):
        return remote(
            outd.at[turn(l, k), rows(l)], landing(l, k).at[:, cols[l]], sd.at[l, k], rd.at[l, k], LINK[l]
        )

    def diag(l, c):
        return remote(outg.at[c, :, cols[l]], rly.at[c, l], sg.at[l, c], rg.at[l, c], LINK[l])

    def relayed(l, k):
        src = rly.at[k // 2, 1 - l, rows(k % 2)]
        return remote(src, landing(l, k).at[:, cols[1 - l]], sq.at[l, k], rq.at[l, k], LINK[l])

    def pieces(s):
        if s in X_STEPS:
            return tuple((FX + l, turn(l, X_STEPS[s])) for l in range(2))
        b, c = (DG, D_STEPS[s]) if s in D_STEPS else (OWN, s - 6)
        return ((b, 2 * c), (b, 2 * c + 1))

    def load(s, side):
        out = []
        for i, (b, k) in enumerate(pieces(s)):
            src = x.at[rows(k)] if (b == OWN and side == 0) else xg.at[b, side, rows(k)]
            out.append(pltpu.make_async_copy(src, xb.at[rows(2 * side + i)], lx.at[side, i]))
        return out

    def take(s):
        if s in X_STEPS:
            for l in range(2):
                own(l, turn(l, X_STEPS[s])).wait_recv()
        elif s in D_STEPS:
            for l in range(2):
                relay(l, D_STEPS[s]).wait_recv()
        if s < 6:
            for b, k in pieces(s):
                hand(b, k).start()
        for c in load(s, 0):
            c.start()
        if s == 1:
            for l in range(2):
                relay(l, 0).start()
                own(l, turn(l, 3)).start()
        if s == 2:
            for l in range(2):
                relay(l, 1).start()
                direct(l, turn(l, 0)).start()

    def take_other(s):
        if s < 6:
            for b, k in pieces(s):
                hand(b, k).wait_recv()
        elif s == 6:
            hand(OWN, 0).wait_recv()
        for c in load(s, 1):
            c.start()

    weights = [
        pltpu.make_async_copy(h, v, lw.at[i])
        for i, (h, v) in enumerate(((wg_h, wg), (wu_h, wu), (wd_h, wd)))
    ]

    def total(r, slot):
        return mine[r] + trecv[slot, r].astype(F32)

    def blocks(n, f):
        def one(i, carry):
            f(pl.multiple_of(i * 16, 16))
            return carry

        lax.fori_loop(0, n, one, 0)

    def settle(p):
        slot = p % 2
        term(p).wait_recv()
        if p in X_STEPS:
            n = X_STEPS[p]
            for l in range(2):

                def f(i, l=l):
                    r = pl.ds(l * PIECE + i, 16)
                    v = total(r, slot)
                    a, b = v[:, :half], v[:, half:]
                    outd[n, r] = (b if l else a).astype(BF16)
                    hold[n, r] = a if l else b

                blocks(PIECE // 16, f)
                if n > 0:
                    direct(l, turn(l, n)).start()
        elif p in D_STEPS:
            n = D_STEPS[p]

            def f(i):
                r = pl.ds(i, 16)
                outg[n, r] = total(r, slot).astype(BF16)

            blocks(8, f)
            for l in range(2):
                diag(l, n).start()
        else:

            def f(i):
                r = pl.ds(i, 16)
                v = total(r, slot)
                hold[0, r] = v[:, :half]
                hold[1, r] = v[:, half:]

            blocks(8, f)

    def pass_on(c):
        for l in range(2):
            diag(1 - l, c).wait_recv()
        for k in (2 * c, 2 * c + 1):
            for l in range(2):

                def f(i, k=k, l=l):
                    r = pl.ds((k % 2) * PIECE + i, 16)
                    v = hold[turn(l, k), pl.ds(l * PIECE + i, 16)] + rly[c, 1 - l, r].astype(F32)
                    rly[c, 1 - l, r] = v.astype(BF16)

                blocks(PIECE // 16, f)
                relayed(l, k).start()

    def gate_up(lo, hi):
        def one(j, carry):
            c = pl.ds(pl.multiple_of(j * GT, GT), GT)
            g = jnp.dot(xb[...], wg[:, c], preferred_element_type=F32)
            u = jnp.dot(xb[...], wu[:, c], preferred_element_type=F32)
            hb[:, c] = (jax.nn.silu(g) * u).astype(BF16)
            return carry

        lax.fori_loop(lo, hi, one, 0)

    def down(lo, hi):
        def one(j, carry):
            c = pl.ds(pl.multiple_of(j * DT, DT), DT)
            t = jnp.dot(hb[...], wd[:, c], preferred_element_type=F32)
            mine[:, c] = t[: 2 * PIECE]
            tsend[:, c] = t[2 * PIECE :].astype(BF16)
            return carry

        lax.fori_loop(lo, hi, one, 0)

    barrier = pltpu.get_barrier_semaphore()
    for mask in (SIB, YN, XN):
        pl.semaphore_signal(barrier, inc=1, device_id={"tp": me ^ mask}, device_id_type=MESH)
    pl.semaphore_wait(barrier, 3)

    for k in range(3):
        for l in range(2):
            own(l, turn(l, k)).start()
    for i in range(2):
        weights[i].start()
    for i in range(2):
        weights[i].wait()
    weights[2].start()
    take(0)
    take_other(0)
    hand(OWN, 0).start()

    def at(s, table):
        for k, fs in table.items():

            @pl.when(s == k)
            def _(fs=fs):
                for f, *args in fs:
                    f(*args)

    after_tiles = {p + 1: [(settle, p)] for p in range(7)}
    after_gate = {s: [(take, s + 1)] for s in range(7)}
    late = {s: [(take_other, s + 1)] for s in range(7)}
    ends = {s: [(term(s).start,)] for s in range(STEPS)}
    ends[3] += after_gate.pop(3) + late.pop(3)
    after_gate.setdefault(3, [])
    after_gate[7] = []
    after_gate[0].append((weights[2].wait,))
    after_gate[5].append((pass_on, 0))
    ends[6].append((pass_on, 1))
    for s in range(1, STEPS):
        after_gate[s].append((term(s - 1).wait_send,))

    def step(s, carry):
        for side in range(2):
            for c in load(0, side):
                c.wait()
        gate_up(0, 3)
        at(s, after_tiles)
        gate_up(3, ff // GT)
        at(s, after_gate)
        down(0, d // DT - 1)
        at(s, late)
        down(d // DT - 1, d // DT)
        at(s, ends)
        return carry

    lax.fori_loop(0, STEPS, step, 0)

    for k in range(2):
        for l in range(2):
            direct(l, k).wait_recv()
            relayed(l, k).wait_recv()
    back = [
        pltpu.make_async_copy(fh.at[l, k], xb.at[rows(2 * l + k)], lf.at[l, k])
        for l in range(2)
        for k in range(2)
    ]
    for c in back:
        c.start()
    term(7).wait_recv()
    for k in range(4):
        for l in range(2):
            direct(l, k).wait_send()
    for c in back:
        c.wait()

    def first(i):
        r = pl.ds(i, 16)
        v = xb[r].astype(F32) + xb[pl.ds(128 + i, 16)].astype(F32)
        outd[0, r] = (hold[0, r] + v[:, :half]).astype(BF16)
        outd[1, r] = (hold[1, r] + v[:, half:]).astype(BF16)

    blocks(8, first)
    outs = [
        pltpu.make_async_copy(outd.at[h], y.at[rows(0, 2), cols[h]], ly.at[0, h]) for h in range(2)
    ]
    for c in outs:
        c.start()
    for k in (2, 3):
        for l in range(2):
            direct(l, k).wait_recv()
            relayed(l, k).wait_recv()

        def last(i, k=k):
            r = pl.ds((k - 2) * PIECE + i, 16)
            q = pl.ds(i, 16)
            v = total(r, 1) + fv[0, k - 2, q].astype(F32) + fv[1, k - 2, q].astype(F32)
            outd[2, r] = v[:, :half].astype(BF16)
            outd[3, r] = v[:, half:].astype(BF16)

        blocks(PIECE // 16, last)
        for h in range(2):
            c = pltpu.make_async_copy(
                outd.at[2 + h, rows(k - 2)], y.at[rows(k), cols[h]], ly.at[k - 1, h]
            )
            c.start()
            outs.append(c)
    for c in outs:
        c.wait()
    term(7).wait_send()
    hand(OWN, 0).wait_send()
    for l in range(2):
        for k in range(4):
            own(l, k).wait_send()
            relayed(l, k).wait_send()
        for r in range(2):
            relay(l, r).wait_send()
            diag(l, r).wait_send()
    for b in (FX, FY, DG):
        for k in range(4):
            hand(b, k).wait_send()


def solution(mesh):
    def step(x, w_gate, w_up, w_down):
        r, d = x.shape
        ff = w_gate.shape[1]
        hbm = pl.BlockSpec(memory_space=pl.ANY)
        dma = pltpu.SemaphoreType.DMA
        half = d // 2
        y, _, _ = pl.pallas_call(
            body,
            out_shape=(
                jax.ShapeDtypeStruct((r, d), BF16),
                jax.ShapeDtypeStruct((4, 2, r, d), BF16),
                jax.ShapeDtypeStruct((2, 2, PIECE, d), BF16),
            ),
            in_specs=[hbm] * 4,
            out_specs=(hbm,) * 3,
            scratch_shapes=[
                pltpu.VMEM((d, ff), BF16),
                pltpu.VMEM((d, ff), BF16),
                pltpu.VMEM((ff, d), BF16),
                pltpu.VMEM((256, d), BF16),
                pltpu.VMEM((256, ff), BF16),
                pltpu.VMEM((128, d), F32),
                pltpu.VMEM((128, d), BF16),
                pltpu.VMEM((2, 128, d), BF16),
                pltpu.VMEM((4, 128, half), BF16),
                pltpu.VMEM((2, 128, d), BF16),
                pltpu.VMEM((2, 2, 128, half), BF16),
                pltpu.VMEM((4, 128, half), F32),
                pltpu.VMEM((2, 2, PIECE, d), BF16),
                dma((2, 4)), dma((2, 4)), dma((2, 2)), dma((2, 2)), dma((4, 4)), dma((4, 4)),
                dma((2,)), dma((2,)), dma((2, 4)), dma((2, 4)), dma((2, 2)), dma((2, 2)),
                dma((2, 4)), dma((2, 4)), dma((2, 2)), dma((3,)), dma((2, 2)), dma((3, 2)),
            ],
            compiler_params=pltpu.CompilerParams(
                collective_id=0, has_side_effects=True, vmem_limit_bytes=67043328
            ),
            cost_estimate=pl.CostEstimate(
                flops=6 * 8 * r * d * ff, bytes_accessed=6 * d * ff + 4 * r * d, transcendentals=8 * r * ff
            ),
            name="mlp",
        )(x, w_gate, w_up, w_down)
        return y

    return jax.shard_map(
        step,
        mesh=mesh,
        in_specs=(P(("dp", "tp"), None), P(None, "tp"), P(None, "tp"), P("tp", None)),
        out_specs=P(("dp", "tp"), None),
        check_vma=False,
    )
```

```python
import jax
import jax.numpy as jnp
from jax import lax
from jax.experimental import pallas as pl
from jax.experimental.pallas import tpu as pltpu
from jax.sharding import PartitionSpec as P

F32 = jnp.float32
BF16 = jnp.bfloat16
MESH = pl.DeviceIdType.MESH

SIB, YN, XN = 1, 2, 4
LINK = (XN, YN)
OWN, FX, FY, DG = 0, 1, 2, 3
PIECE = 64
STEPS = 8
X_STEPS = {0: 0, 1: 1, 2: 2, 4: 3}
D_STEPS = {3: 0, 5: 1}
SWAP = (1, 0, 3, 2)
GT = 256
DT = 1024


def body(
    x, wg_h, wu_h, wd_h, y, xg, fh,
    wg, wu, wd, xb, hb, mine, tsend, trecv, outd, outg, rly, hold, fv,
    so, ro, sr, rr, ss, rs, st, rt, sd, rd, sg, rg, sq, rq, lx, lw, lf, ly,
):
    me = lax.axis_index("tp")
    d = x.shape[1]
    half = d // 2
    ff = wg.shape[1]
    cols = (pl.ds(0, half), pl.ds(half, half))

    def remote(src, dst, send, recv, mask):
        return pltpu.make_async_remote_copy(
            src_ref=src, dst_ref=dst, send_sem=send, recv_sem=recv,
            device_id={"tp": me ^ mask}, device_id_type=MESH,
        )

    def rows(k, n=1):
        return pl.ds(k * PIECE, n * PIECE)

    def turn(l, k):
        return SWAP[k] if l else k

    def own(l, k):
        return remote(x.at[rows(k)], xg.at[FX + l, 0, rows(k)], so.at[l, k], ro.at[l, k], LINK[l])

    def relay(l, r):
        k = 2 * r + 1 - l
        return remote(
            xg.at[FY - l, 0, rows(k)], xg.at[DG, 0, rows(k)], sr.at[l, r], rr.at[l, r], LINK[l]
        )

    def hand(b, k):
        if b == OWN:
            return remote(x, xg.at[OWN, 1], ss.at[0, 0], rs.at[0, 0], SIB)
        return remote(xg.at[b, 0, rows(k)], xg.at[b, 1, rows(k)], ss.at[b, k], rs.at[b, k], SIB)

    def term(s):
        slot = s % 2
        return remote(tsend, trecv.at[slot], st.at[slot], rt.at[slot], SIB)

    def landing(l, k):
        return fh.at[l, k] if k < 2 else fv.at[l, k - 2]

    def direct(l, k):
        return remote(
            outd.at[turn(l, k), rows(l)], landing(l, k).at[:, cols[l]], sd.at[l, k], rd.at[l, k], LINK[l]
        )

    def diag(l, c):
        return remote(outg.at[c, :, cols[l]], rly.at[c, l], sg.at[l, c], rg.at[l, c], LINK[l])

    def relayed(l, k):
        src = rly.at[k // 2, 1 - l, rows(k % 2)]
        return remote(src, landing(l, k).at[:, cols[1 - l]], sq.at[l, k], rq.at[l, k], LINK[l])

    def pieces(s):
        if s in X_STEPS:
            return tuple((FX + l, turn(l, X_STEPS[s])) for l in range(2))
        b, c = (DG, D_STEPS[s]) if s in D_STEPS else (OWN, s - 6)
        return ((b, 2 * c), (b, 2 * c + 1))

    def load(s, side):
        out = []
        for i, (b, k) in enumerate(pieces(s)):
            src = x.at[rows(k)] if (b == OWN and side == 0) else xg.at[b, side, rows(k)]
            out.append(pltpu.make_async_copy(src, xb.at[rows(2 * side + i)], lx.at[side, i]))
        return out

    def take(s):
        if s in X_STEPS:
            for l in range(2):
                own(l, turn(l, X_STEPS[s])).wait_recv()
        elif s in D_STEPS:
            for l in range(2):
                relay(l, D_STEPS[s]).wait_recv()
        if s < 6:
            for b, k in pieces(s):
                hand(b, k).start()
        for c in load(s, 0):
            c.start()
        if s == 1:
            for l in range(2):
                relay(l, 0).start()
                own(l, turn(l, 3)).start()
        if s == 2:
            for l in range(2):
                relay(l, 1).start()
                direct(l, turn(l, 0)).start()

    def take_other(s):
        if s < 6:
            for b, k in pieces(s):
                hand(b, k).wait_recv()
        elif s == 6:
            hand(OWN, 0).wait_recv()
        for c in load(s, 1):
            c.start()

    weights = [
        pltpu.make_async_copy(h, v, lw.at[i])
        for i, (h, v) in enumerate(((wg_h, wg), (wu_h, wu), (wd_h, wd)))
    ]

    def total(r, slot):
        return mine[r] + trecv[slot, r].astype(F32)

    def blocks(n, f):
        def one(i, carry):
            f(pl.multiple_of(i * 16, 16))
            return carry

        lax.fori_loop(0, n, one, 0)

    def settle(p):
        slot = p % 2
        term(p).wait_recv()
        if p in X_STEPS:
            n = X_STEPS[p]
            for l in range(2):

                def f(i, l=l):
                    r = pl.ds(l * PIECE + i, 16)
                    v = total(r, slot)
                    a, b = v[:, :half], v[:, half:]
                    outd[n, r] = (b if l else a).astype(BF16)
                    hold[n, r] = a if l else b

                blocks(PIECE // 16, f)
                if n > 0:
                    direct(l, turn(l, n)).start()
        elif p in D_STEPS:
            n = D_STEPS[p]

            def f(i):
                r = pl.ds(i, 16)
                outg[n, r] = total(r, slot).astype(BF16)

            blocks(8, f)
            for l in range(2):
                diag(l, n).start()
        else:

            def f(i):
                r = pl.ds(i, 16)
                v = total(r, slot)
                hold[0, r] = v[:, :half]
                hold[1, r] = v[:, half:]

            blocks(8, f)

    def pass_on(c):
        for l in range(2):
            diag(1 - l, c).wait_recv()
        for k in (2 * c, 2 * c + 1):
            for l in range(2):

                def f(i, k=k, l=l):
                    r = pl.ds((k % 2) * PIECE + i, 16)
                    v = hold[turn(l, k), pl.ds(l * PIECE + i, 16)] + rly[c, 1 - l, r].astype(F32)
                    rly[c, 1 - l, r] = v.astype(BF16)

                blocks(PIECE // 16, f)
                relayed(l, k).start()

    def gate_up(lo, hi):
        def one(j, carry):
            c = pl.ds(pl.multiple_of(j * GT, GT), GT)
            g = jnp.dot(xb[...], wg[:, c], preferred_element_type=F32)
            u = jnp.dot(xb[...], wu[:, c], preferred_element_type=F32)
            hb[:, c] = (jax.nn.silu(g) * u).astype(BF16)
            return carry

        lax.fori_loop(lo, hi, one, 0, unroll=True)

    def down(lo, hi):
        def one(j, carry):
            c = pl.ds(pl.multiple_of(j * DT, DT), DT)
            t = jnp.dot(hb[...], wd[:, c], preferred_element_type=F32)
            mine[:, c] = t[: 2 * PIECE]
            tsend[:, c] = t[2 * PIECE :].astype(BF16)
            return carry

        lax.fori_loop(lo, hi, one, 0, unroll=True)

    barrier = pltpu.get_barrier_semaphore()
    for mask in (SIB, YN, XN):
        pl.semaphore_signal(barrier, inc=1, device_id={"tp": me ^ mask}, device_id_type=MESH)
    pl.semaphore_wait(barrier, 3)

    for k in range(3):
        for l in range(2):
            own(l, turn(l, k)).start()
    for i in range(2):
        weights[i].start()
    for i in range(2):
        weights[i].wait()
    weights[2].start()
    take(0)
    take_other(0)
    hand(OWN, 0).start()

    def at(s, table):
        for k, fs in table.items():

            @pl.when(s == k)
            def _(fs=fs):
                for f, *args in fs:
                    f(*args)

    after_tiles = {p + 1: [(settle, p)] for p in range(7)}
    after_gate = {s: [(take, s + 1)] for s in range(7)}
    late = {s: [(take_other, s + 1)] for s in range(7)}
    ends = {s: [(term(s).start,)] for s in range(STEPS)}
    after_gate[7] = []
    after_gate[0].append((weights[2].wait,))
    after_gate[6].append((pass_on, 0))
    ends[7].append((pass_on, 1))
    for s in range(1, STEPS):
        after_gate[s].append((term(s - 1).wait_send,))

    def step(s, carry):
        for side in range(2):
            for c in load(0, side):
                c.wait()
        gate_up(0, 3)
        at(s, after_tiles)
        gate_up(3, ff // GT)
        at(s, after_gate)
        down(0, d // DT - 1)
        at(s, late)
        down(d // DT - 1, d // DT)
        at(s, ends)
        return carry

    lax.fori_loop(0, STEPS, step, 0)

    for k in range(2):
        for l in range(2):
            direct(l, k).wait_recv()
            relayed(l, k).wait_recv()
    back = [
        pltpu.make_async_copy(fh.at[l, k], xb.at[rows(2 * l + k)], lf.at[l, k])
        for l in range(2)
        for k in range(2)
    ]
    for c in back:
        c.start()
    term(7).wait_recv()
    for k in range(4):
        for l in range(2):
            direct(l, k).wait_send()
    for c in back:
        c.wait()

    def first(i):
        r = pl.ds(i, 16)
        v = xb[r].astype(F32) + xb[pl.ds(128 + i, 16)].astype(F32)
        outd[0, r] = (hold[0, r] + v[:, :half]).astype(BF16)
        outd[1, r] = (hold[1, r] + v[:, half:]).astype(BF16)

    blocks(8, first)
    outs = [
        pltpu.make_async_copy(outd.at[h], y.at[rows(0, 2), cols[h]], ly.at[0, h]) for h in range(2)
    ]
    for c in outs:
        c.start()
    for k in (2, 3):
        for l in range(2):
            direct(l, k).wait_recv()
            relayed(l, k).wait_recv()

        def last(i, k=k):
            r = pl.ds((k - 2) * PIECE + i, 16)
            q = pl.ds(i, 16)
            v = total(r, 1) + fv[0, k - 2, q].astype(F32) + fv[1, k - 2, q].astype(F32)
            outd[2, r] = v[:, :half].astype(BF16)
            outd[3, r] = v[:, half:].astype(BF16)

        blocks(PIECE // 16, last)
        for h in range(2):
            c = pltpu.make_async_copy(
                outd.at[2 + h, rows(k - 2)], y.at[rows(k), cols[h]], ly.at[k - 1, h]
            )
            c.start()
            outs.append(c)
    for c in outs:
        c.wait()
    term(7).wait_send()
    hand(OWN, 0).wait_send()
    for l in range(2):
        for k in range(4):
            own(l, k).wait_send()
            relayed(l, k).wait_send()
        for r in range(2):
            relay(l, r).wait_send()
            diag(l, r).wait_send()
    for b in (FX, FY, DG):
        for k in range(4):
            hand(b, k).wait_send()


def solution(mesh):
    def step(x, w_gate, w_up, w_down):
        r, d = x.shape
        ff = w_gate.shape[1]
        hbm = pl.BlockSpec(memory_space=pl.ANY)
        dma = pltpu.SemaphoreType.DMA
        half = d // 2
        y, _, _ = pl.pallas_call(
            body,
            out_shape=(
                jax.ShapeDtypeStruct((r, d), BF16),
                jax.ShapeDtypeStruct((4, 2, r, d), BF16),
                jax.ShapeDtypeStruct((2, 2, PIECE, d), BF16),
            ),
            in_specs=[hbm] * 4,
            out_specs=(hbm,) * 3,
            scratch_shapes=[
                pltpu.VMEM((d, ff), BF16),
                pltpu.VMEM((d, ff), BF16),
                pltpu.VMEM((ff, d), BF16),
                pltpu.VMEM((256, d), BF16),
                pltpu.VMEM((256, ff), BF16),
                pltpu.VMEM((128, d), F32),
                pltpu.VMEM((128, d), BF16),
                pltpu.VMEM((2, 128, d), BF16),
                pltpu.VMEM((4, 128, half), BF16),
                pltpu.VMEM((2, 128, d), BF16),
                pltpu.VMEM((2, 2, 128, half), BF16),
                pltpu.VMEM((4, 128, half), F32),
                pltpu.VMEM((2, 2, PIECE, d), BF16),
                dma((2, 4)), dma((2, 4)), dma((2, 2)), dma((2, 2)), dma((4, 4)), dma((4, 4)),
                dma((2,)), dma((2,)), dma((2, 4)), dma((2, 4)), dma((2, 2)), dma((2, 2)),
                dma((2, 4)), dma((2, 4)), dma((2, 2)), dma((3,)), dma((2, 2)), dma((3, 2)),
            ],
            compiler_params=pltpu.CompilerParams(
                collective_id=0, has_side_effects=True, vmem_limit_bytes=67043328
            ),
            cost_estimate=pl.CostEstimate(
                flops=6 * 8 * r * d * ff, bytes_accessed=6 * d * ff + 4 * r * d, transcendentals=8 * r * ff
            ),
            name="mlp",
        )(x, w_gate, w_up, w_down)
        return y

    return jax.shard_map(
        step,
        mesh=mesh,
        in_specs=(P(("dp", "tp"), None), P(None, "tp"), P(None, "tp"), P("tp", None)),
        out_specs=P(("dp", "tp"), None),
        check_vma=False,
    )
```

```python
import jax
import jax.numpy as jnp
from jax import lax
from jax.experimental import pallas as pl
from jax.experimental.pallas import tpu as pltpu
from jax.sharding import PartitionSpec as P

F32 = jnp.float32
BF16 = jnp.bfloat16
MESH = pl.DeviceIdType.MESH

SIB, YN, XN = 1, 2, 4
LINK = (XN, YN)
OWN, FX, FY, DG = 0, 1, 2, 3
PIECE = 64
STEPS = 8
X_STEPS = {0: 0, 1: 1, 2: 2, 4: 3}
D_STEPS = {3: 0, 5: 1}
SWAP = (1, 0, 3, 2)
GT = 256
DT = 1024


def body(
    x, wg_h, wu_h, wd_h, y, xg, fh,
    wg, wu, wd, xb, hb, mine, tsend, trecv, outg, rly, hold, fv,
    so, ro, sr, rr, ss, rs, st, rt, sd, rd, sg, rg, sq, rq, lx, lw, lf,
):
    me = lax.axis_index("tp")
    d = x.shape[1]
    half = d // 2
    ff = wg.shape[1]
    cols = (pl.ds(0, half), pl.ds(half, half))

    def remote(src, dst, send, recv, mask):
        return pltpu.make_async_remote_copy(
            src_ref=src, dst_ref=dst, send_sem=send, recv_sem=recv,
            device_id={"tp": me ^ mask}, device_id_type=MESH,
        )

    def rows(k, n=1):
        return pl.ds(k * PIECE, n * PIECE)

    def turn(l, k):
        return SWAP[k] if l else k

    def own(l, k):
        return remote(x.at[rows(k)], xg.at[FX + l, 0, rows(k)], so.at[l, k], ro.at[l, k], LINK[l])

    def relay(l, r):
        k = 2 * r + 1 - l
        return remote(
            xg.at[FY - l, 0, rows(k)], xg.at[DG, 0, rows(k)], sr.at[l, r], rr.at[l, r], LINK[l]
        )

    def hand(b, k):
        if b == OWN:
            return remote(x, xg.at[OWN, 1], ss.at[0, 0], rs.at[0, 0], SIB)
        return remote(xg.at[b, 0, rows(k)], xg.at[b, 1, rows(k)], ss.at[b, k], rs.at[b, k], SIB)

    def term(s):
        slot = s % 2
        return remote(tsend, trecv.at[slot], st.at[slot], rt.at[slot], SIB)

    def landing(l, k, cols):
        return fh.at[l, k, :, cols] if k < 2 else fv.at[l, k - 2, :, cols]

    def direct(l, k):
        return remote(
            y.at[rows(2 * (turn(l, k) // 2) + l), cols[turn(l, k) % 2]], landing(l, k, cols[l]), sd.at[l, k], rd.at[l, k], LINK[l]
        )

    def diag(l, c):
        return remote(outg.at[c, :, cols[l]], rly.at[c, l], sg.at[l, c], rg.at[l, c], LINK[l])

    def relayed(l, k):
        src = rly.at[k // 2, 1 - l, rows(k % 2)]
        return remote(src, landing(l, k, cols[1 - l]), sq.at[l, k], rq.at[l, k], LINK[l])

    def pieces(s):
        if s in X_STEPS:
            return tuple((FX + l, turn(l, X_STEPS[s])) for l in range(2))
        b, c = (DG, D_STEPS[s]) if s in D_STEPS else (OWN, s - 6)
        return ((b, 2 * c), (b, 2 * c + 1))

    def load(s, side):
        out = []
        for i, (b, k) in enumerate(pieces(s)):
            src = x.at[rows(k)] if (b == OWN and side == 0) else xg.at[b, side, rows(k)]
            out.append(pltpu.make_async_copy(src, xb.at[rows(2 * side + i)], lx.at[side, i]))
        return out

    def take(s):
        if s in X_STEPS:
            for l in range(2):
                own(l, turn(l, X_STEPS[s])).wait_recv()
        elif s in D_STEPS:
            for l in range(2):
                relay(l, D_STEPS[s]).wait_recv()
        if s < 6:
            for b, k in pieces(s):
                hand(b, k).start()
        for c in load(s, 0):
            c.start()
        if s == 1:
            for l in range(2):
                relay(l, 0).start()
                own(l, turn(l, 3)).start()
        if s == 2:
            for l in range(2):
                relay(l, 1).start()
                direct(l, turn(l, 0)).start()

    def take_other(s):
        if s < 6:
            for b, k in pieces(s):
                hand(b, k).wait_recv()
        elif s == 6:
            hand(OWN, 0).wait_recv()
        for c in load(s, 1):
            c.start()

    weights = [
        pltpu.make_async_copy(h, v, lw.at[i])
        for i, (h, v) in enumerate(((wg_h, wg), (wu_h, wu), (wd_h, wd)))
    ]

    def total(r, slot):
        return mine[r] + trecv[slot, r].astype(F32)

    def blocks(n, f):
        def one(i, carry):
            f(pl.multiple_of(i * 16, 16))
            return carry

        lax.fori_loop(0, n, one, 0)

    def settle(p):
        slot = p % 2
        term(p).wait_recv()
        if p in X_STEPS:
            n = X_STEPS[p]
            for l in range(2):

                def f(i, l=l):
                    r = pl.ds(l * PIECE + i, 16)
                    v = total(r, slot)
                    a, b = v[:, :half], v[:, half:]
                    q = pl.ds((n // 2) * 2 * PIECE + l * PIECE + i, 16)
                    y[q, cols[n % 2]] = (b if l else a).astype(BF16)
                    hold[n, r] = a if l else b

                blocks(PIECE // 16, f)
                if n > 0:
                    direct(l, turn(l, n)).start()
        elif p in D_STEPS:
            n = D_STEPS[p]

            def f(i):
                r = pl.ds(i, 16)
                outg[n, r] = total(r, slot).astype(BF16)

            blocks(8, f)
            for l in range(2):
                diag(l, n).start()
        else:

            def f(i):
                r = pl.ds(i, 16)
                v = total(r, slot)
                hold[0, r] = v[:, :half]
                hold[1, r] = v[:, half:]

            blocks(8, f)

    def pass_on(c):
        for l in range(2):
            diag(1 - l, c).wait_recv()
        for k in (2 * c, 2 * c + 1):
            for l in range(2):

                def f(i, k=k, l=l):
                    r = pl.ds((k % 2) * PIECE + i, 16)
                    v = hold[turn(l, k), pl.ds(l * PIECE + i, 16)] + rly[c, 1 - l, r].astype(F32)
                    rly[c, 1 - l, r] = v.astype(BF16)

                blocks(PIECE // 16, f)
                relayed(l, k).start()

    def gate_up(lo, hi):
        def one(j, carry):
            c = pl.ds(pl.multiple_of(j * GT, GT), GT)
            g = jnp.dot(xb[...], wg[:, c], preferred_element_type=F32)
            u = jnp.dot(xb[...], wu[:, c], preferred_element_type=F32)
            hb[:, c] = (jax.nn.silu(g) * u).astype(BF16)
            return carry

        lax.fori_loop(lo, hi, one, 0, unroll=True)

    def down(lo, hi):
        def one(j, carry):
            c = pl.ds(pl.multiple_of(j * DT, DT), DT)
            t = jnp.dot(hb[...], wd[:, c], preferred_element_type=F32)
            mine[:, c] = t[: 2 * PIECE]
            tsend[:, c] = t[2 * PIECE :].astype(BF16)
            return carry

        lax.fori_loop(lo, hi, one, 0, unroll=True)

    barrier = pltpu.get_barrier_semaphore()
    for mask in (SIB, YN, XN):
        pl.semaphore_signal(barrier, inc=1, device_id={"tp": me ^ mask}, device_id_type=MESH)
    pl.semaphore_wait(barrier, 3)

    for k in range(3):
        for l in range(2):
            own(l, turn(l, k)).start()
    for i in range(2):
        weights[i].start()
    for i in range(2):
        weights[i].wait()
    weights[2].start()
    take(0)
    take_other(0)
    hand(OWN, 0).start()

    def at(s, table):
        for k, fs in table.items():

            @pl.when(s == k)
            def _(fs=fs):
                for f, *args in fs:
                    f(*args)

    after_tiles = {p + 1: [(settle, p)] for p in range(7)}
    after_gate = {s: [(take, s + 1)] for s in range(7)}
    late = {s: [(take_other, s + 1)] for s in range(7)}
    ends = {s: [(term(s).start,)] for s in range(STEPS)}
    after_gate[7] = []
    after_gate[0].append((weights[2].wait,))
    after_gate[6].append((pass_on, 0))
    ends[7].append((pass_on, 1))
    for s in range(1, STEPS):
        after_gate[s].append((term(s - 1).wait_send,))

    def step(s, carry):
        for side in range(2):
            for c in load(0, side):
                c.wait()
        gate_up(0, 3)
        at(s, after_tiles)
        gate_up(3, ff // GT)
        at(s, after_gate)
        down(0, d // DT - 1)
        at(s, late)
        down(d // DT - 1, d // DT)
        at(s, ends)
        return carry

    lax.fori_loop(0, STEPS, step, 0)

    for k in range(4):
        for l in range(2):
            direct(l, k).wait_send()
    for k in range(2):
        for l in range(2):
            direct(l, k).wait_recv()
            relayed(l, k).wait_recv()
        back = [
            pltpu.make_async_copy(fh.at[l, k], xb.at[rows(2 * l + k)], lf.at[l, k])
            for l in range(2)
        ]
        for c in back:
            c.start()
        for c in back:
            c.wait()

        def first(i, k=k):
            r = pl.ds(k * PIECE + i, 16)
            v = xb[r].astype(F32) + xb[pl.ds((2 + k) * PIECE + i, 16)].astype(F32)
            y[r, cols[0]] = (hold[0, r] + v[:, :half]).astype(BF16)
            y[r, cols[1]] = (hold[1, r] + v[:, half:]).astype(BF16)

        blocks(PIECE // 16, first)
    term(7).wait_recv()
    for k in (2, 3):
        for l in range(2):
            direct(l, k).wait_recv()
            relayed(l, k).wait_recv()

        def last(i, k=k):
            q = pl.ds(i, 16)
            v = fv[0, k - 2, q].astype(F32) + fv[1, k - 2, q].astype(F32)
            v = total(pl.ds((k - 2) * PIECE + i, 16), 1) + v
            y[pl.ds(k * PIECE + i, 16)] = v.astype(BF16)

        blocks(PIECE // 16, last)
    term(7).wait_send()
    hand(OWN, 0).wait_send()
    for l in range(2):
        for k in range(4):
            own(l, k).wait_send()
            relayed(l, k).wait_send()
        for r in range(2):
            relay(l, r).wait_send()
            diag(l, r).wait_send()
    for b in (FX, FY, DG):
        for k in range(4):
            hand(b, k).wait_send()


def solution(mesh):
    def step(x, w_gate, w_up, w_down):
        r, d = x.shape
        ff = w_gate.shape[1]
        hbm = pl.BlockSpec(memory_space=pl.ANY)
        dma = pltpu.SemaphoreType.DMA
        half = d // 2
        y, _, _ = pl.pallas_call(
            body,
            out_shape=(
                pltpu.VMEM((r, d), BF16),
                jax.ShapeDtypeStruct((4, 2, r, d), BF16),
                jax.ShapeDtypeStruct((2, 2, PIECE, d), BF16),
            ),
            in_specs=[hbm] * 4,
            out_specs=(pl.BlockSpec(memory_space=pltpu.VMEM), hbm, hbm),
            scratch_shapes=[
                pltpu.VMEM((d, ff), BF16),
                pltpu.VMEM((d, ff), BF16),
                pltpu.VMEM((ff, d), BF16),
                pltpu.VMEM((256, d), BF16),
                pltpu.VMEM((256, ff), BF16),
                pltpu.VMEM((128, d), F32),
                pltpu.VMEM((128, d), BF16),
                pltpu.VMEM((2, 128, d), BF16),
                pltpu.VMEM((2, 128, d), BF16),
                pltpu.VMEM((2, 2, 128, half), BF16),
                pltpu.VMEM((4, 128, half), F32),
                pltpu.VMEM((2, 2, PIECE, d), BF16),
                dma((2, 4)), dma((2, 4)), dma((2, 2)), dma((2, 2)), dma((4, 4)), dma((4, 4)),
                dma((2,)), dma((2,)), dma((2, 4)), dma((2, 4)), dma((2, 2)), dma((2, 2)),
                dma((2, 4)), dma((2, 4)), dma((2, 2)), dma((3,)), dma((2, 2)),
            ],
            compiler_params=pltpu.CompilerParams(
                collective_id=0, has_side_effects=True, vmem_limit_bytes=64487424
            ),
            cost_estimate=pl.CostEstimate(
                flops=6 * 8 * r * d * ff, bytes_accessed=6 * d * ff + 4 * r * d, transcendentals=8 * r * ff
            ),
            name="mlp",
        )(x, w_gate, w_up, w_down)
        def put(src, dst, sems):
            out = [
                pltpu.make_async_copy(src.at[pl.ds(32 * i, 32)], dst.at[pl.ds(32 * i, 32)], sems.at[i])
                for i in range(8)
            ]
            for c in out:
                c.start()
            for c in out:
                c.wait()

        return pl.pallas_call(
            put,
            out_shape=jax.ShapeDtypeStruct((r, d), BF16),
            in_specs=[pl.BlockSpec(memory_space=pltpu.VMEM)],
            out_specs=hbm,
            scratch_shapes=[dma((8,))],
            compiler_params=pltpu.CompilerParams(vmem_limit_bytes=4194304),
            name="put",
        )(y)

    return jax.shard_map(
        step,
        mesh=mesh,
        in_specs=(P(("dp", "tp"), None), P(None, "tp"), P(None, "tp"), P("tp", None)),
        out_specs=P(("dp", "tp"), None),
        check_vma=False,
    )
```

```python
import jax
import jax.numpy as jnp
from jax import lax
from jax.experimental import pallas as pl
from jax.experimental.pallas import tpu as pltpu
from jax.sharding import PartitionSpec as P

F32 = jnp.float32
BF16 = jnp.bfloat16
MESH = pl.DeviceIdType.MESH

SIB, YN, XN = 1, 2, 4
LINK = (XN, YN)
OWN, FX, FY, DG = 0, 1, 2, 3
PIECE = 64
STEPS = 8
X_STEPS = {0: 0, 1: 1, 2: 2, 4: 3}
D_STEPS = {3: 0, 5: 1}
SWAP = (1, 0, 3, 2)
GT = 256
DT = 1024


def body(
    x, wg_h, wu_h, wd_h, y, xg, fh,
    wg, wu, wd, xb, hb, mine, tsend, trecv, outg, rly, hold, fv,
    sent, ro, rr, rs, rt, rg, rf, lx, lw,
):
    me = lax.axis_index("tp")
    d = x.shape[1]
    half = d // 2
    ff = wg.shape[1]
    cols = (pl.ds(0, half), pl.ds(half, half))

    def remote(src, dst, send, recv, mask):
        return pltpu.make_async_remote_copy(
            src_ref=src, dst_ref=dst, send_sem=send, recv_sem=recv,
            device_id={"tp": me ^ mask}, device_id_type=MESH,
        )

    def rows(k, n=1):
        return pl.ds(k * PIECE, n * PIECE)

    def drain(sem, n):
        ref = {1: xg.at[0, 0, rows(0)], 2: xg.at[0, 0, rows(0, 2)], 4: xg.at[0, 0], 32: xg}[n]
        pltpu.make_async_copy(ref, ref, sem).wait()

    def turn(l, k):
        return SWAP[k] if l else k

    def own(l, k):
        n = turn(l, k)
        return remote(x.at[rows(k)], xg.at[FX + l, 0, rows(k)], sent.at[0], ro.at[n], LINK[l])

    def relay(l, r):
        k = 2 * r + 1 - l
        return remote(
            xg.at[FY - l, 0, rows(k)], xg.at[DG, 0, rows(k)], sent.at[0], rr.at[r], LINK[l]
        )

    def hand_own():
        return remote(x, xg.at[OWN, 1], sent.at[0], rs.at[2], SIB)

    def hand(s):
        return [
            remote(xg.at[b, 0, rows(k)], xg.at[b, 1, rows(k)], sent.at[0], rs.at[s % 2], SIB)
            for b, k in pieces(s)
        ]

    def term(s):
        return remote(tsend, trecv.at[s % 2], sent.at[1], rt.at[s % 2], SIB)

    def landing(c):
        return fv if c else fh

    def direct(l, c):
        src = y.at[rows(2 * c, 2), cols[l]]
        return remote(src, landing(c).at[l, :, cols[l]], sent.at[2], rf.at[c], LINK[l])

    def diag(l, c):
        return remote(outg.at[c, :, cols[l]], rly.at[c, l], sent.at[0], rg.at[c], LINK[l])

    def relayed(l, c, k, n, sem):
        dst = landing(c).at[l, rows(k, n), cols[1 - l]]
        return remote(rly.at[c, 1 - l, rows(k, n)], dst, sent.at[3], rf.at[sem], LINK[l])

    RELAYED = (((0, 2, 0),), ((0, 1, 2), (1, 1, 3)))

    def pieces(s):
        if s in X_STEPS:
            return tuple((FX + l, turn(l, X_STEPS[s])) for l in range(2))
        b, c = (DG, D_STEPS[s]) if s in D_STEPS else (OWN, s - 6)
        return ((b, 2 * c), (b, 2 * c + 1))

    def load(s, side):
        out = []
        for i, (b, k) in enumerate(pieces(s)):
            src = x.at[rows(k)] if (b == OWN and side == 0) else xg.at[b, side, rows(k)]
            out.append(pltpu.make_async_copy(src, xb.at[rows(2 * side + i)], lx.at[0]))
        return out

    def take(s):
        if s in X_STEPS:
            drain(ro.at[X_STEPS[s]], 2)
        elif s in D_STEPS:
            drain(rr.at[D_STEPS[s]], 2)
        if s < 6:
            for c in hand(s):
                c.start()
        for c in load(s, 0):
            c.start()
        if s == 1:
            for l in range(2):
                relay(l, 0).start()
                own(l, turn(l, 3)).start()
        if s == 2:
            for l in range(2):
                relay(l, 1).start()

    def take_other(s):
        if s < 6:
            drain(rs.at[s % 2], 2)
        elif s == 6:
            hand_own().wait_recv()
        for c in load(s, 1):
            c.start()

    weights = [
        pltpu.make_async_copy(h, v, lw.at[i])
        for i, (h, v) in enumerate(((wg_h, wg), (wu_h, wu), (wd_h, wd)))
    ]

    def total(r, slot):
        return mine[r] + trecv[slot, r].astype(F32)

    def blocks(n, f):
        def one(i, carry):
            f(pl.multiple_of(i * 16, 16))
            return carry

        lax.fori_loop(0, n, one, 0)

    def settle(p):
        slot = p % 2
        term(p).wait_recv()
        if p in X_STEPS:
            n = X_STEPS[p]
            for l in range(2):

                def f(i, l=l):
                    v = total(pl.ds(l * PIECE + i, 16), slot)
                    a, b = v[:, :half], v[:, half:]
                    r = pl.ds(turn(l, n) * PIECE + i, 16)
                    y[r, cols[l]] = (b if l else a).astype(BF16)
                    hold[l, r] = a if l else b

                blocks(PIECE // 16, f)
            if n % 2:
                for l in range(2):
                    direct(l, n // 2).start()
        elif p in D_STEPS:
            n = D_STEPS[p]

            def f(i):
                r = pl.ds(i, 16)
                outg[n, r] = total(r, slot).astype(BF16)

            blocks(8, f)
            for l in range(2):
                diag(l, n).start()
        else:

            def f(i):
                r = pl.ds(i, 16)
                v = total(r, slot)
                hold[0, r] = v[:, :half]
                hold[1, r] = v[:, half:]

            blocks(8, f)

    def pass_on(c):
        drain(rg.at[c], 2)
        for k, n, sem in RELAYED[c]:
            for l in range(2):

                def f(i, k=k, l=l):
                    r = pl.ds(k * PIECE + i, 16)
                    v = hold[l, pl.ds((2 * c + k) * PIECE + i, 16)] + rly[c, 1 - l, r].astype(F32)
                    rly[c, 1 - l, r] = v.astype(BF16)

                blocks(n * PIECE // 16, f)
                relayed(l, c, k, n, sem).start()

    def gate_up(lo, hi):
        def one(j, carry):
            c = pl.ds(pl.multiple_of(j * GT, GT), GT)
            g = jnp.dot(xb[...], wg[:, c], preferred_element_type=F32)
            u = jnp.dot(xb[...], wu[:, c], preferred_element_type=F32)
            hb[:, c] = (jax.nn.silu(g) * u).astype(BF16)
            return carry

        lax.fori_loop(lo, hi, one, 0, unroll=True)

    def down(lo, hi):
        def one(j, carry):
            c = pl.ds(pl.multiple_of(j * DT, DT), DT)
            t = jnp.dot(hb[...], wd[:, c], preferred_element_type=F32)
            mine[:, c] = t[: 2 * PIECE]
            tsend[:, c] = t[2 * PIECE :].astype(BF16)
            return carry

        lax.fori_loop(lo, hi, one, 0, unroll=True)

    barrier = pltpu.get_barrier_semaphore()
    for mask in (SIB, YN, XN):
        pl.semaphore_signal(barrier, inc=1, device_id={"tp": me ^ mask}, device_id_type=MESH)
    pl.semaphore_wait(barrier, 3)

    for k in range(3):
        for l in range(2):
            own(l, turn(l, k)).start()
    for i in range(2):
        weights[i].start()
    for i in range(2):
        weights[i].wait()
    weights[2].start()
    take(0)
    take_other(0)
    hand_own().start()

    def at(s, table):
        for k, fs in table.items():

            @pl.when(s == k)
            def _(fs=fs):
                for f, *args in fs:
                    f(*args)

    after_tiles = {p + 1: [(settle, p)] for p in range(7)}
    after_gate = {s: [(take, s + 1)] for s in range(7)}
    late = {s: [(take_other, s + 1)] for s in range(7)}
    ends = {s: [(term(s).start,)] for s in range(STEPS)}
    after_gate[7] = []
    after_gate[0].append((weights[2].wait,))
    after_gate[6].append((pass_on, 0))
    ends[7].append((pass_on, 1))
    for s in range(1, STEPS):
        after_gate[s].append((term(s - 1).wait_send,))

    def step(s, carry):
        drain(lx.at[0], 4)
        gate_up(0, 3)
        at(s, after_tiles)
        gate_up(3, ff // GT)
        at(s, after_gate)
        down(0, d // DT - 1)
        at(s, late)
        down(d // DT - 1, d // DT)
        at(s, ends)
        return carry

    lax.fori_loop(0, STEPS, step, 0)

    drain(sent.at[2], 4)
    drain(rf.at[0], 4)
    back = [pltpu.make_async_copy(fh.at[l], xb.at[rows(2 * l, 2)], lx.at[0]) for l in range(2)]
    for c in back:
        c.start()
    drain(lx.at[0], 4)

    def first(i):
        r = pl.ds(i, 16)
        v = xb[r].astype(F32) + xb[pl.ds(2 * PIECE + i, 16)].astype(F32)
        y[r, cols[0]] = (hold[0, r] + v[:, :half]).astype(BF16)
        y[r, cols[1]] = (hold[1, r] + v[:, half:]).astype(BF16)

    blocks(2 * PIECE // 16, first)
    term(7).wait_recv()
    drain(rf.at[1], 2)

    def add_direct(i):
        r = pl.ds(i, 16)
        for c, l in zip(cols, range(2)):
            mine[r, c] += trecv[1, r, c].astype(F32) + fv[l, r, c].astype(F32)

    blocks(2 * PIECE // 16, add_direct)
    for k, n, sem in RELAYED[1]:
        drain(rf.at[sem], 1)

        def add_relayed(i, k=k):
            r = pl.ds(k * PIECE + i, 16)
            for c, l in zip(cols, range(2)):
                v = mine[r, c] + fv[1 - l, r, c].astype(F32)
                y[pl.ds((2 + k) * PIECE + i, 16), c] = v.astype(BF16)

        blocks(n * PIECE // 16, add_relayed)
    term(7).wait_send()
    drain(sent.at[0], 32)
    drain(sent.at[3], 4)


def solution(mesh):
    def step(x, w_gate, w_up, w_down):
        r, d = x.shape
        ff = w_gate.shape[1]
        hbm = pl.BlockSpec(memory_space=pl.ANY)
        dma = pltpu.SemaphoreType.DMA
        half = d // 2
        y, _, _ = pl.pallas_call(
            body,
            out_shape=(
                pltpu.VMEM((r, d), BF16),
                jax.ShapeDtypeStruct((4, 2, r, d), BF16),
                jax.ShapeDtypeStruct((2, 2 * PIECE, d), BF16),
            ),
            in_specs=[hbm] * 4,
            out_specs=(pl.BlockSpec(memory_space=pltpu.VMEM), hbm, hbm),
            scratch_shapes=[
                pltpu.VMEM((d, ff), BF16),
                pltpu.VMEM((d, ff), BF16),
                pltpu.VMEM((ff, d), BF16),
                pltpu.VMEM((256, d), BF16),
                pltpu.VMEM((256, ff), BF16),
                pltpu.VMEM((128, d), F32),
                pltpu.VMEM((128, d), BF16),
                pltpu.VMEM((2, 128, d), BF16),
                pltpu.VMEM((2, 128, d), BF16),
                pltpu.VMEM((2, 2, 128, half), BF16),
                pltpu.VMEM((2, 256, half), F32),
                pltpu.VMEM((2, 2 * PIECE, d), BF16),
                dma((4,)), dma((4,)), dma((2,)), dma((3,)), dma((2,)), dma((2,)), dma((4,)), dma((1,)), dma((3,)),
            ],
            compiler_params=pltpu.CompilerParams(
                collective_id=0, has_side_effects=True, vmem_limit_bytes=64487424
            ),
            cost_estimate=pl.CostEstimate(
                flops=6 * 8 * r * d * ff, bytes_accessed=6 * d * ff + 4 * r * d, transcendentals=8 * r * ff
            ),
            name="mlp",
        )(x, w_gate, w_up, w_down)
        def put(src, dst, sem):
            c = pltpu.make_async_copy(src, dst, sem.at[0])
            c.start()
            c.wait()

        return pl.pallas_call(
            put,
            out_shape=jax.ShapeDtypeStruct((r, d), BF16),
            in_specs=[pl.BlockSpec(memory_space=pltpu.VMEM)],
            out_specs=hbm,
            scratch_shapes=[dma((1,))],
            compiler_params=pltpu.CompilerParams(vmem_limit_bytes=4194304),
            name="put",
        )(y)

    return jax.shard_map(
        step,
        mesh=mesh,
        in_specs=(P(("dp", "tp"), None), P(None, "tp"), P(None, "tp"), P("tp", None)),
        out_specs=P(("dp", "tp"), None),
        check_vma=False,
    )
```

```python
import jax
import jax.numpy as jnp
from jax import lax
from jax.experimental import pallas as pl
from jax.experimental.pallas import tpu as pltpu
from jax.sharding import PartitionSpec as P

F32 = jnp.float32
BF16 = jnp.bfloat16
MESH = pl.DeviceIdType.MESH

SIB, YN, XN = 1, 2, 4
LINK = (XN, YN)
OWN, FX, FY, DG = 0, 1, 2, 3
PIECE = 64
STEPS = 8
X_STEPS = {0: 0, 1: 1, 2: 2, 4: 3}
D_STEPS = {3: 0, 5: 1}
SWAP = (1, 0, 3, 2)
GT = 256
DT = 1024


def body(
    x, wg_h, wu_h, wd_h, y, xg, fh,
    wg, wu, wd, xb, hb, mine, tsend, trecv, outg, rly, hold, fv,
    sent, ro, rr, rs, rt, rg, rf, lx, lw, late,
):
    me = lax.axis_index("tp")
    d = x.shape[1]
    half = d // 2
    ff = wg.shape[1]
    cols = (pl.ds(0, half), pl.ds(half, half))

    def remote(src, dst, send, recv, mask):
        return pltpu.make_async_remote_copy(
            src_ref=src, dst_ref=dst, send_sem=send, recv_sem=recv,
            device_id={"tp": me ^ mask}, device_id_type=MESH,
        )

    def rows(k, n=1):
        return pl.ds(k * PIECE, n * PIECE)

    def drain(sem, n):
        ref = {1: xg.at[0, 0, rows(0)], 2: xg.at[0, 0, rows(0, 2)], 4: xg.at[0, 0], 32: xg}[n]
        pltpu.make_async_copy(ref, ref, sem).wait()

    def turn(l, k):
        return SWAP[k] if l else k

    def own(l, k):
        n = turn(l, k)
        return remote(x.at[rows(k)], xg.at[FX + l, 0, rows(k)], sent.at[0], ro.at[n], LINK[l])

    def relay(l, r):
        k = 2 * r + 1 - l
        return remote(
            xg.at[FY - l, 0, rows(k)], xg.at[DG, 0, rows(k)], sent.at[0], rr.at[r], LINK[l]
        )

    def hand_own():
        return remote(x, xg.at[OWN, 1], sent.at[0], rs.at[2], SIB)

    def hand(s):
        return [
            remote(xg.at[b, 0, rows(k)], xg.at[b, 1, rows(k)], sent.at[0], rs.at[s % 2], SIB)
            for b, k in pieces(s)
        ]

    def term(s):
        return remote(tsend, trecv.at[s % 2], sent.at[1], rt.at[s % 2], SIB)

    def landing(c):
        return fv if c else fh

    def direct(l, c):
        src = y.at[rows(2 * c, 2), cols[l]]
        return remote(src, landing(c).at[l, :, cols[l]], sent.at[2], rf.at[c], LINK[l])

    def diag(l, c):
        return remote(outg.at[c, :, cols[l]], rly.at[c, l], sent.at[0], rg.at[c], LINK[l])

    def relayed(l, c, k, n, sem):
        dst = landing(c).at[l, rows(k, n), cols[1 - l]]
        return remote(rly.at[c, 1 - l, rows(k, n)], dst, sent.at[3], rf.at[sem], LINK[l])

    RELAYED = (((0, 2, 0),), ((0, 1, 2), (1, 1, 3)))

    def pieces(s):
        if s in X_STEPS:
            return tuple((FX + l, turn(l, X_STEPS[s])) for l in range(2))
        b, c = (DG, D_STEPS[s]) if s in D_STEPS else (OWN, s - 6)
        return ((b, 2 * c), (b, 2 * c + 1))

    def load(s, side):
        out = []
        for i, (b, k) in enumerate(pieces(s)):
            src = x.at[rows(k)] if (b == OWN and side == 0) else xg.at[b, side, rows(k)]
            out.append(pltpu.make_async_copy(src, xb.at[rows(2 * side + i)], lx.at[0]))
        return out

    def take(s):
        if s in X_STEPS:
            drain(ro.at[X_STEPS[s]], 2)
        elif s in D_STEPS:
            drain(rr.at[D_STEPS[s]], 2)
        if s < 6:
            for c in hand(s):
                c.start()
        for c in load(s, 0):
            c.start()
        if s == 1:
            for l in range(2):
                relay(l, 0).start()
                own(l, turn(l, 3)).start()
        if s == 2:
            for l in range(2):
                relay(l, 1).start()

    def take_other(s):
        if s < 6:
            drain(rs.at[s % 2], 2)
        elif s == 6:
            hand_own().wait_recv()
        for c in load(s, 1):
            c.start()

    weights = [
        pltpu.make_async_copy(h, v, lw.at[i])
        for i, (h, v) in enumerate(((wg_h, wg), (wu_h, wu), (wd_h, wd)))
    ]

    def total(r, slot):
        return mine[r] + trecv[slot, r].astype(F32)

    def blocks(n, f):
        def one(i, carry):
            f(pl.multiple_of(i * 16, 16))
            return carry

        lax.fori_loop(0, n, one, 0)

    def settle(p):
        slot = p % 2
        term(p).wait_recv()
        if p in X_STEPS:
            n = X_STEPS[p]
            for l in range(2):

                def f(i, l=l):
                    v = total(pl.ds(l * PIECE + i, 16), slot)
                    a, b = v[:, :half], v[:, half:]
                    r = pl.ds(turn(l, n) * PIECE + i, 16)
                    y[r, cols[l]] = (b if l else a).astype(BF16)
                    hold[l, r] = a if l else b

                blocks(PIECE // 16, f)
            if n % 2:
                for l in range(2):
                    direct(l, n // 2).start()
        elif p in D_STEPS:
            n = D_STEPS[p]

            def f(i):
                r = pl.ds(i, 16)
                outg[n, r] = total(r, slot).astype(BF16)

            blocks(8, f)
            for l in range(2):
                diag(l, n).start()
        else:

            def f(i):
                r = pl.ds(i, 16)
                v = total(r, slot)
                hold[0, r] = v[:, :half]
                hold[1, r] = v[:, half:]

            blocks(8, f)

    def pass_on(c):
        drain(rg.at[c], 2)
        for k, n, sem in RELAYED[c]:
            for l in range(2):

                def f(i, k=k, l=l):
                    r = pl.ds(k * PIECE + i, 16)
                    v = hold[l, pl.ds((2 * c + k) * PIECE + i, 16)] + rly[c, 1 - l, r].astype(F32)
                    rly[c, 1 - l, r] = v.astype(BF16)

                blocks(n * PIECE // 16, f)
                relayed(l, c, k, n, sem).start()

    def gate_up(lo, hi):
        def one(j, carry):
            c = pl.ds(pl.multiple_of(j * GT, GT), GT)
            g = jnp.dot(xb[...], wg[:, c], preferred_element_type=F32)
            u = jnp.dot(xb[...], wu[:, c], preferred_element_type=F32)
            hb[:, c] = (jax.nn.silu(g) * u).astype(BF16)
            return carry

        lax.fori_loop(lo, hi, one, 0, unroll=True)

    def down(lo, hi):
        def one(j, carry):
            c = pl.ds(pl.multiple_of(j * DT, DT), DT)
            t = jnp.dot(hb[...], wd[:, c], preferred_element_type=F32)
            mine[:, c] = t[: 2 * PIECE]
            tsend[:, c] = t[2 * PIECE :].astype(BF16)
            return carry

        lax.fori_loop(lo, hi, one, 0, unroll=True)

    chip = me // 2
    middle = (chip == 1) | (chip == 2)
    barrier = pltpu.get_barrier_semaphore()

    def greet(sem, mask):
        pl.semaphore_signal(sem, inc=1, device_id={"tp": me ^ mask}, device_id_type=MESH)

    greet(barrier, SIB)

    @pl.when(chip != 3)
    def _():
        for mask in LINK:
            greet(barrier, mask)

    @pl.when(middle)
    def _():
        pl.semaphore_wait(barrier, 2)

    @pl.when(jnp.logical_not(middle))
    def _():
        pl.semaphore_wait(barrier, 3)

    @pl.when(chip == 3)
    def _():
        for mask in LINK:
            greet(late, mask)

    def first_pieces(l):
        for k in range(3):
            own(l, turn(l, k)).start()

    to_last = [chip ^ (LINK[l] // 2) == 3 for l in range(2)]
    for l in range(2):

        @pl.when(jnp.logical_not(to_last[l]))
        def _(l=l):
            first_pieces(l)

    for i in range(2):
        weights[i].start()
    for l in range(2):

        @pl.when(to_last[l])
        def _(l=l):
            pl.semaphore_wait(late, 1)
            first_pieces(l)

    for i in range(2):
        weights[i].wait()
    weights[2].start()
    take(0)
    take_other(0)
    hand_own().start()

    def at(s, table):
        for k, fs in table.items():

            @pl.when(s == k)
            def _(fs=fs):
                for f, *args in fs:
                    f(*args)

    after_tiles = {p + 1: [(settle, p)] for p in range(7)}
    after_gate = {s: [(take, s + 1)] for s in range(7)}
    after_tile = {s: [(take_other, s + 1)] for s in range(7)}
    ends = {s: [(term(s).start,)] for s in range(STEPS)}
    after_gate[7] = []
    after_gate[0].append((weights[2].wait,))
    after_gate[6].append((pass_on, 0))
    ends[7].append((pass_on, 1))
    for s in range(1, STEPS):
        after_gate[s].append((term(s - 1).wait_send,))

    def step(s, carry):
        drain(lx.at[0], 4)
        gate_up(0, 3)
        at(s, after_tiles)
        gate_up(3, ff // GT)
        at(s, after_gate)
        down(0, d // DT - 1)
        at(s, after_tile)
        down(d // DT - 1, d // DT)
        at(s, ends)
        return carry

    lax.fori_loop(0, STEPS, step, 0)

    drain(sent.at[2], 4)
    drain(rf.at[0], 4)
    back = [pltpu.make_async_copy(fh.at[l], xb.at[rows(2 * l, 2)], lx.at[0]) for l in range(2)]
    for c in back:
        c.start()
    drain(lx.at[0], 4)

    def first(i):
        r = pl.ds(i, 16)
        v = xb[r].astype(F32) + xb[pl.ds(2 * PIECE + i, 16)].astype(F32)
        y[r, cols[0]] = (hold[0, r] + v[:, :half]).astype(BF16)
        y[r, cols[1]] = (hold[1, r] + v[:, half:]).astype(BF16)

    blocks(2 * PIECE // 16, first)
    term(7).wait_recv()
    drain(rf.at[1], 2)

    def add_direct(i):
        r = pl.ds(i, 16)
        for c, l in zip(cols, range(2)):
            mine[r, c] += trecv[1, r, c].astype(F32) + fv[l, r, c].astype(F32)

    blocks(2 * PIECE // 16, add_direct)
    for k, n, sem in RELAYED[1]:
        drain(rf.at[sem], 1)

        def add_relayed(i, k=k):
            r = pl.ds(k * PIECE + i, 16)
            for c, l in zip(cols, range(2)):
                v = mine[r, c] + fv[1 - l, r, c].astype(F32)
                y[pl.ds((2 + k) * PIECE + i, 16), c] = v.astype(BF16)

        blocks(n * PIECE // 16, add_relayed)
    term(7).wait_send()
    drain(sent.at[0], 32)
    drain(sent.at[3], 4)


def solution(mesh):
    def step(x, w_gate, w_up, w_down):
        r, d = x.shape
        ff = w_gate.shape[1]
        hbm = pl.BlockSpec(memory_space=pl.ANY)
        dma = pltpu.SemaphoreType.DMA
        half = d // 2
        y, _, _ = pl.pallas_call(
            body,
            out_shape=(
                pltpu.VMEM((r, d), BF16),
                jax.ShapeDtypeStruct((4, 2, r, d), BF16),
                jax.ShapeDtypeStruct((2, 2 * PIECE, d), BF16),
            ),
            in_specs=[hbm] * 4,
            out_specs=(pl.BlockSpec(memory_space=pltpu.VMEM), hbm, hbm),
            scratch_shapes=[
                pltpu.VMEM((d, ff), BF16),
                pltpu.VMEM((d, ff), BF16),
                pltpu.VMEM((ff, d), BF16),
                pltpu.VMEM((256, d), BF16),
                pltpu.VMEM((256, ff), BF16),
                pltpu.VMEM((128, d), F32),
                pltpu.VMEM((128, d), BF16),
                pltpu.VMEM((2, 128, d), BF16),
                pltpu.VMEM((2, 128, d), BF16),
                pltpu.VMEM((2, 2, 128, half), BF16),
                pltpu.VMEM((2, 256, half), F32),
                pltpu.VMEM((2, 2 * PIECE, d), BF16),
                dma((4,)), dma((4,)), dma((2,)), dma((3,)), dma((2,)), dma((2,)), dma((4,)), dma((1,)), dma((3,)),
                pltpu.SemaphoreType.REGULAR,
            ],
            compiler_params=pltpu.CompilerParams(
                collective_id=0, has_side_effects=True, vmem_limit_bytes=64487424
            ),
            cost_estimate=pl.CostEstimate(
                flops=6 * 8 * r * d * ff, bytes_accessed=6 * d * ff + 4 * r * d, transcendentals=8 * r * ff
            ),
            name="mlp",
        )(x, w_gate, w_up, w_down)
        def put(src, dst, sem):
            c = pltpu.make_async_copy(src, dst, sem.at[0])
            c.start()
            c.wait()

        return pl.pallas_call(
            put,
            out_shape=jax.ShapeDtypeStruct((r, d), BF16),
            in_specs=[pl.BlockSpec(memory_space=pltpu.VMEM)],
            out_specs=hbm,
            scratch_shapes=[dma((1,))],
            compiler_params=pltpu.CompilerParams(vmem_limit_bytes=4194304),
            name="put",
        )(y)

    return jax.shard_map(
        step,
        mesh=mesh,
        in_specs=(P(("dp", "tp"), None), P(None, "tp"), P(None, "tp"), P("tp", None)),
        out_specs=P(("dp", "tp"), None),
        check_vma=False,
    )
```

```python
import jax
import jax.numpy as jnp
from jax import lax
from jax.experimental import pallas as pl
from jax.experimental.pallas import tpu as pltpu
from jax.sharding import PartitionSpec as P

F32 = jnp.float32
BF16 = jnp.bfloat16
MESH = pl.DeviceIdType.MESH

SIB, YN, XN = 1, 2, 4
LINK = (XN, YN)
OWN, FX, FY, DG = 0, 1, 2, 3
PIECE = 64
STEPS = 8
X_STEPS = {0: 0, 1: 1, 2: 2, 4: 3}
D_STEPS = {3: 0, 5: 1}
SWAP = (1, 0, 3, 2)
GT = 256
DT = 1024


def body(
    x, wg_h, wu_h, wd_h, y, xg, fh,
    wg, wu, wd, xb, hb, mine, tsend, trecv, outg, rly, hold, fv,
    sent, ro, rr, rs, rt, rg, rf, lx, lw, late,
):
    me = lax.axis_index("tp")
    d = x.shape[1]
    half = d // 2
    ff = wg.shape[1]
    cols = (pl.ds(0, half), pl.ds(half, half))

    def remote(src, dst, send, recv, mask):
        return pltpu.make_async_remote_copy(
            src_ref=src, dst_ref=dst, send_sem=send, recv_sem=recv,
            device_id={"tp": me ^ mask}, device_id_type=MESH,
        )

    def rows(k, n=1):
        return pl.ds(k * PIECE, n * PIECE)

    def drain(sem, n):
        ref = {1: xg.at[0, 0, rows(0)], 2: xg.at[0, 0, rows(0, 2)], 4: xg.at[0, 0], 32: xg}[n]
        pltpu.make_async_copy(ref, ref, sem).wait()

    def turn(l, k):
        return SWAP[k] if l else k

    def own(l, k):
        n = turn(l, k)
        return remote(x.at[rows(k)], xg.at[FX + l, 0, rows(k)], sent.at[0], ro.at[n], LINK[l])

    def relay(l, r):
        k = 2 * r + 1 - l
        return remote(
            xg.at[FY - l, 0, rows(k)], xg.at[DG, 0, rows(k)], sent.at[0], rr.at[r], LINK[l]
        )

    def hand_own():
        return remote(x, xg.at[OWN, 1], sent.at[0], rs.at[2], SIB)

    def hand(s):
        return [
            remote(xg.at[b, 0, rows(k)], xg.at[b, 1, rows(k)], sent.at[0], rs.at[s % 2], SIB)
            for b, k in pieces(s)
        ]

    def term(s):
        return remote(tsend, trecv.at[s % 2], sent.at[1], rt.at[s % 2], SIB)

    def landing(c):
        return fv if c else fh

    def direct(l, c):
        src = y.at[rows(2 * c, 2), cols[l]]
        return remote(src, landing(c).at[l, :, cols[l]], sent.at[2], rf.at[c], LINK[l])

    def diag(l, c):
        return remote(outg.at[c, :, cols[l]], rly.at[c, l], sent.at[0], rg.at[c], LINK[l])

    def relayed(l, c, k, n, sem):
        dst = landing(c).at[l, rows(k, n), cols[1 - l]]
        return remote(rly.at[c, 1 - l, rows(k, n)], dst, sent.at[3], rf.at[sem], LINK[l])

    RELAYED = (((0, 2, 0),), ((0, 1, 2), (1, 1, 3)))

    def pieces(s):
        if s in X_STEPS:
            return tuple((FX + l, turn(l, X_STEPS[s])) for l in range(2))
        b, c = (DG, D_STEPS[s]) if s in D_STEPS else (OWN, s - 6)
        return ((b, 2 * c), (b, 2 * c + 1))

    def load(s, side):
        out = []
        for i, (b, k) in enumerate(pieces(s)):
            src = x.at[rows(k)] if (b == OWN and side == 0) else xg.at[b, side, rows(k)]
            out.append(pltpu.make_async_copy(src, xb.at[rows(2 * side + i)], lx.at[0]))
        return out

    def take(s):
        if s in X_STEPS:
            drain(ro.at[X_STEPS[s]], 2)
        elif s in D_STEPS:
            drain(rr.at[D_STEPS[s]], 2)
        if s < 6:
            for c in hand(s):
                c.start()
        for c in load(s, 0):
            c.start()
        if s == 1:
            for l in range(2):
                relay(l, 0).start()
                own(l, turn(l, 3)).start()
        if s == 2:
            for l in range(2):
                relay(l, 1).start()

    def take_other(s):
        if s < 6:
            drain(rs.at[s % 2], 2)
        elif s == 6:
            hand_own().wait_recv()
        for c in load(s, 1):
            c.start()

    weights = [
        pltpu.make_async_copy(h, v, lw.at[i])
        for i, (h, v) in enumerate(((wg_h, wg), (wu_h, wu), (wd_h, wd)))
    ]

    def total(r, slot):
        return mine[r] + trecv[slot, r].astype(F32)

    def blocks(n, f):
        def one(i, carry):
            f(pl.multiple_of(i * 16, 16))
            return carry

        lax.fori_loop(0, n, one, 0)

    def settle(p):
        slot = p % 2
        term(p).wait_recv()
        if p in X_STEPS:
            n = X_STEPS[p]
            for l in range(2):

                def f(i, l=l):
                    v = total(pl.ds(l * PIECE + i, 16), slot)
                    a, b = v[:, :half], v[:, half:]
                    r = pl.ds(turn(l, n) * PIECE + i, 16)
                    y[r, cols[l]] = (b if l else a).astype(BF16)
                    hold[l, r] = a if l else b

                blocks(PIECE // 16, f)
            if n % 2:
                for l in range(2):
                    direct(l, n // 2).start()
        elif p in D_STEPS:
            n = D_STEPS[p]

            def f(i):
                r = pl.ds(i, 16)
                outg[n, r] = total(r, slot).astype(BF16)

            blocks(8, f)
            for l in range(2):
                diag(l, n).start()
        else:

            def f(i):
                r = pl.ds(i, 16)
                v = total(r, slot)
                hold[0, r] = v[:, :half]
                hold[1, r] = v[:, half:]

            blocks(8, f)

    def pass_on(c):
        drain(rg.at[c], 2)
        for k, n, sem in RELAYED[c]:
            for l in range(2):

                def f(i, k=k, l=l):
                    r = pl.ds(k * PIECE + i, 16)
                    v = hold[l, pl.ds((2 * c + k) * PIECE + i, 16)] + rly[c, 1 - l, r].astype(F32)
                    rly[c, 1 - l, r] = v.astype(BF16)

                blocks(n * PIECE // 16, f)
                relayed(l, c, k, n, sem).start()

    def gate_up(lo, hi):
        def one(j, carry):
            c = pl.ds(pl.multiple_of(j * GT, GT), GT)
            g = jnp.dot(xb[...], wg[:, c], preferred_element_type=F32)
            u = jnp.dot(xb[...], wu[:, c], preferred_element_type=F32)
            hb[:, c] = (jax.nn.silu(g) * u).astype(BF16)
            return carry

        lax.fori_loop(lo, hi, one, 0, unroll=True)

    def down(lo, hi):
        def one(j, carry):
            c = pl.ds(pl.multiple_of(j * DT, DT), DT)
            t = jnp.dot(hb[...], wd[:, c], preferred_element_type=F32)
            mine[:, c] = t[: 2 * PIECE]
            tsend[:, c] = t[2 * PIECE :].astype(BF16)
            return carry

        lax.fori_loop(lo, hi, one, 0, unroll=True)

    chip = me // 2
    middle = (chip == 1) | (chip == 2)
    barrier = pltpu.get_barrier_semaphore()

    def greet(sem, mask):
        pl.semaphore_signal(sem, inc=1, device_id={"tp": me ^ mask}, device_id_type=MESH)

    greet(barrier, SIB)

    @pl.when(chip != 3)
    def _():
        for mask in LINK:
            greet(barrier, mask)

    @pl.when(middle)
    def _():
        pl.semaphore_wait(barrier, 2)

    @pl.when(jnp.logical_not(middle))
    def _():
        pl.semaphore_wait(barrier, 3)

    @pl.when(chip == 3)
    def _():
        for mask in LINK:
            greet(late, mask)

    def first_pieces(l):
        for k in range(3):
            own(l, turn(l, k)).start()

    to_last = [chip ^ (LINK[l] // 2) == 3 for l in range(2)]
    behind = middle & (me % 2 == 1)
    for l in range(2):

        @pl.when(jnp.logical_not(to_last[l] | behind))
        def _(l=l):
            first_pieces(l)

    for i in range(2):
        weights[i].start()

    @pl.when(middle)
    def _():
        pl.semaphore_wait(late, 1)

    for l in range(2):

        @pl.when(to_last[l] | behind)
        def _(l=l):
            first_pieces(l)

    for i in range(2):
        weights[i].wait()
    weights[2].start()
    take(0)
    take_other(0)
    hand_own().start()

    def at(s, table):
        for k, fs in table.items():

            @pl.when(s == k)
            def _(fs=fs):
                for f, *args in fs:
                    f(*args)

    after_tiles = {p + 1: [(settle, p)] for p in range(7)}
    after_gate = {s: [(take, s + 1)] for s in range(7)}
    after_tile = {s: [(take_other, s + 1)] for s in range(7)}
    ends = {s: [(term(s).start,)] for s in range(STEPS)}
    after_gate[7] = []
    after_gate[0].append((weights[2].wait,))
    after_gate[6].append((pass_on, 0))
    ends[7].append((pass_on, 1))
    for s in range(1, STEPS):
        after_gate[s].append((term(s - 1).wait_send,))

    def step(s, carry):
        drain(lx.at[0], 4)
        gate_up(0, 3)
        at(s, after_tiles)
        gate_up(3, ff // GT)
        at(s, after_gate)
        down(0, d // DT - 1)
        at(s, after_tile)
        down(d // DT - 1, d // DT)
        at(s, ends)
        return carry

    lax.fori_loop(0, STEPS, step, 0)

    drain(sent.at[2], 4)
    drain(rf.at[0], 4)
    back = [pltpu.make_async_copy(fh.at[l], xb.at[rows(2 * l, 2)], lx.at[0]) for l in range(2)]
    for c in back:
        c.start()
    drain(lx.at[0], 4)

    def first(i):
        r = pl.ds(i, 16)
        v = xb[r].astype(F32) + xb[pl.ds(2 * PIECE + i, 16)].astype(F32)
        y[r, cols[0]] = (hold[0, r] + v[:, :half]).astype(BF16)
        y[r, cols[1]] = (hold[1, r] + v[:, half:]).astype(BF16)

    blocks(2 * PIECE // 16, first)
    term(7).wait_recv()
    drain(rf.at[1], 2)

    def add_direct(i):
        r = pl.ds(i, 16)
        for c, l in zip(cols, range(2)):
            mine[r, c] += trecv[1, r, c].astype(F32) + fv[l, r, c].astype(F32)

    blocks(2 * PIECE // 16, add_direct)
    for k, n, sem in RELAYED[1]:
        drain(rf.at[sem], 1)

        def add_relayed(i, k=k):
            r = pl.ds(k * PIECE + i, 16)
            for c, l in zip(cols, range(2)):
                v = mine[r, c] + fv[1 - l, r, c].astype(F32)
                y[pl.ds((2 + k) * PIECE + i, 16), c] = v.astype(BF16)

        blocks(n * PIECE // 16, add_relayed)
    term(7).wait_send()
    drain(sent.at[0], 32)
    drain(sent.at[3], 4)


def solution(mesh):
    def step(x, w_gate, w_up, w_down):
        r, d = x.shape
        ff = w_gate.shape[1]
        hbm = pl.BlockSpec(memory_space=pl.ANY)
        dma = pltpu.SemaphoreType.DMA
        half = d // 2
        y, _, _ = pl.pallas_call(
            body,
            out_shape=(
                pltpu.VMEM((r, d), BF16),
                jax.ShapeDtypeStruct((4, 2, r, d), BF16),
                jax.ShapeDtypeStruct((2, 2 * PIECE, d), BF16),
            ),
            in_specs=[hbm] * 4,
            out_specs=(pl.BlockSpec(memory_space=pltpu.VMEM), hbm, hbm),
            scratch_shapes=[
                pltpu.VMEM((d, ff), BF16),
                pltpu.VMEM((d, ff), BF16),
                pltpu.VMEM((ff, d), BF16),
                pltpu.VMEM((256, d), BF16),
                pltpu.VMEM((256, ff), BF16),
                pltpu.VMEM((128, d), F32),
                pltpu.VMEM((128, d), BF16),
                pltpu.VMEM((2, 128, d), BF16),
                pltpu.VMEM((2, 128, d), BF16),
                pltpu.VMEM((2, 2, 128, half), BF16),
                pltpu.VMEM((2, 256, half), F32),
                pltpu.VMEM((2, 2 * PIECE, d), BF16),
                dma((4,)), dma((4,)), dma((2,)), dma((3,)), dma((2,)), dma((2,)), dma((4,)), dma((1,)), dma((3,)),
                pltpu.SemaphoreType.REGULAR,
            ],
            compiler_params=pltpu.CompilerParams(
                collective_id=0, has_side_effects=True, vmem_limit_bytes=64487424
            ),
            cost_estimate=pl.CostEstimate(
                flops=6 * 8 * r * d * ff, bytes_accessed=6 * d * ff + 4 * r * d, transcendentals=8 * r * ff
            ),
            name="mlp",
        )(x, w_gate, w_up, w_down)
        def put(src, dst, sem):
            c = pltpu.make_async_copy(src, dst, sem.at[0])
            c.start()
            c.wait()

        return pl.pallas_call(
            put,
            out_shape=jax.ShapeDtypeStruct((r, d), BF16),
            in_specs=[pl.BlockSpec(memory_space=pltpu.VMEM)],
            out_specs=hbm,
            scratch_shapes=[dma((1,))],
            compiler_params=pltpu.CompilerParams(vmem_limit_bytes=4194304),
            name="put",
        )(y)

    return jax.shard_map(
        step,
        mesh=mesh,
        in_specs=(P(("dp", "tp"), None), P(None, "tp"), P(None, "tp"), P("tp", None)),
        out_specs=P(("dp", "tp"), None),
        check_vma=False,
    )
```

```python
import jax
import jax.numpy as jnp
from jax import lax
from jax.experimental import pallas as pl
from jax.experimental.pallas import tpu as pltpu
from jax.sharding import PartitionSpec as P

F32 = jnp.float32
BF16 = jnp.bfloat16
MESH = pl.DeviceIdType.MESH

SIB, YN, XN = 1, 2, 4
LINK = (XN, YN)
OWN, FX, FY, DG = 0, 1, 2, 3
PIECE = 64
FEW = 16
STEPS = 8
X_STEPS = {0: 0, 1: 1, 2: 2, 4: 3}
D_STEPS = {3: 0, 5: 1}
SWAP = (1, 0, 3, 2)
GT = 256
DT = 1024


def body(
    x, wg_h, wu_h, wd_h, y, xg, fh,
    wg, wu, wd, xb, hb, mine, tsend, trecv, outg, rly, hold, fv,
    sent, ro, rr, rs, rt, rg, rf, lx, lw, late,
):
    me = lax.axis_index("tp")
    d = x.shape[1]
    half = d // 2
    ff = wg.shape[1]
    cols = (pl.ds(0, half), pl.ds(half, half))

    def remote(src, dst, send, recv, mask):
        return pltpu.make_async_remote_copy(
            src_ref=src, dst_ref=dst, send_sem=send, recv_sem=recv,
            device_id={"tp": me ^ mask}, device_id_type=MESH,
        )

    def rows(k, n=1):
        return pl.ds(k * PIECE, n * PIECE)

    def drain(sem, n):
        ref = {1: xg.at[0, 0, rows(0)], 2: xg.at[0, 0, rows(0, 2)], 4: xg.at[0, 0], 32: xg}[n]
        pltpu.make_async_copy(ref, ref, sem).wait()

    def turn(l, k):
        return SWAP[k] if l else k

    def own(l, k, lo=0, hi=PIECE):
        r = pl.ds(k * PIECE + lo, hi - lo)
        return remote(x.at[r], xg.at[FX + l, 0, r], sent.at[0], ro.at[turn(l, k)], LINK[l])

    def relay(l, r):
        k = 2 * r + 1 - l
        return remote(
            xg.at[FY - l, 0, rows(k)], xg.at[DG, 0, rows(k)], sent.at[0], rr.at[r], LINK[l]
        )

    def hand_own():
        return remote(x, xg.at[OWN, 1], sent.at[0], rs.at[2], SIB)

    def hand(s):
        return [
            remote(xg.at[b, 0, rows(k)], xg.at[b, 1, rows(k)], sent.at[0], rs.at[s % 2], SIB)
            for b, k in pieces(s)
        ]

    def term(s):
        return remote(tsend, trecv.at[s % 2], sent.at[1], rt.at[s % 2], SIB)

    def landing(c):
        return fv if c else fh

    def direct(l, c):
        src = y.at[rows(2 * c, 2), cols[l]]
        return remote(src, landing(c).at[l, :, cols[l]], sent.at[2], rf.at[c], LINK[l])

    def diag(l, c):
        return remote(outg.at[c, :, cols[l]], rly.at[c, l], sent.at[0], rg.at[c], LINK[l])

    def relayed(l, c, k, n, sem):
        dst = landing(c).at[l, rows(k, n), cols[1 - l]]
        return remote(rly.at[c, 1 - l, rows(k, n)], dst, sent.at[3], rf.at[sem], LINK[l])

    RELAYED = (((0, 2, 0),), ((0, 1, 2), (1, 1, 3)))

    def pieces(s):
        if s in X_STEPS:
            return tuple((FX + l, turn(l, X_STEPS[s])) for l in range(2))
        b, c = (DG, D_STEPS[s]) if s in D_STEPS else (OWN, s - 6)
        return ((b, 2 * c), (b, 2 * c + 1))

    def load(s, side):
        out = []
        for i, (b, k) in enumerate(pieces(s)):
            src = x.at[rows(k)] if (b == OWN and side == 0) else xg.at[b, side, rows(k)]
            out.append(pltpu.make_async_copy(src, xb.at[rows(2 * side + i)], lx.at[0]))
        return out

    def take(s):
        if s in X_STEPS:
            drain(ro.at[X_STEPS[s]], 2)
        elif s in D_STEPS:
            drain(rr.at[D_STEPS[s]], 2)
        if s < 6:
            for c in hand(s):
                c.start()
        for c in load(s, 0):
            c.start()
        if s == 1:
            for l in range(2):
                relay(l, 0).start()
                own(l, turn(l, 3)).start()
        if s == 2:
            for l in range(2):
                relay(l, 1).start()

    def take_other(s):
        if s < 6:
            drain(rs.at[s % 2], 2)
        elif s == 6:
            hand_own().wait_recv()
        for c in load(s, 1):
            c.start()

    weights = [
        pltpu.make_async_copy(h, v, lw.at[i])
        for i, (h, v) in enumerate(((wg_h, wg), (wu_h, wu), (wd_h, wd)))
    ]

    def total(r, slot):
        return mine[r] + trecv[slot, r].astype(F32)

    def blocks(n, f):
        def one(i, carry):
            f(pl.multiple_of(i * 16, 16))
            return carry

        lax.fori_loop(0, n, one, 0)

    def settle(p):
        slot = p % 2
        term(p).wait_recv()
        if p in X_STEPS:
            n = X_STEPS[p]
            for l in range(2):

                def f(i, l=l):
                    v = total(pl.ds(l * PIECE + i, 16), slot)
                    a, b = v[:, :half], v[:, half:]
                    r = pl.ds(turn(l, n) * PIECE + i, 16)
                    y[r, cols[l]] = (b if l else a).astype(BF16)
                    hold[l, r] = a if l else b

                blocks(PIECE // 16, f)
            if n % 2:
                for l in range(2):
                    direct(l, n // 2).start()
        elif p in D_STEPS:
            n = D_STEPS[p]

            def f(i):
                r = pl.ds(i, 16)
                outg[n, r] = total(r, slot).astype(BF16)

            blocks(8, f)
            for l in range(2):
                diag(l, n).start()
        else:

            def f(i):
                r = pl.ds(i, 16)
                v = total(r, slot)
                hold[0, r] = v[:, :half]
                hold[1, r] = v[:, half:]

            blocks(8, f)

    def pass_on(c):
        drain(rg.at[c], 2)
        for k, n, sem in RELAYED[c]:
            for l in range(2):

                def f(i, k=k, l=l):
                    r = pl.ds(k * PIECE + i, 16)
                    v = hold[l, pl.ds((2 * c + k) * PIECE + i, 16)] + rly[c, 1 - l, r].astype(F32)
                    rly[c, 1 - l, r] = v.astype(BF16)

                blocks(n * PIECE // 16, f)
                relayed(l, c, k, n, sem).start()

    def gate_up(lo, hi):
        def one(j, carry):
            c = pl.ds(pl.multiple_of(j * GT, GT), GT)
            g = jnp.dot(xb[...], wg[:, c], preferred_element_type=F32)
            u = jnp.dot(xb[...], wu[:, c], preferred_element_type=F32)
            hb[:, c] = (jax.nn.silu(g) * u).astype(BF16)
            return carry

        lax.fori_loop(lo, hi, one, 0, unroll=True)

    def down(lo, hi):
        def one(j, carry):
            c = pl.ds(pl.multiple_of(j * DT, DT), DT)
            t = jnp.dot(hb[...], wd[:, c], preferred_element_type=F32)
            mine[:, c] = t[: 2 * PIECE]
            tsend[:, c] = t[2 * PIECE :].astype(BF16)
            return carry

        lax.fori_loop(lo, hi, one, 0, unroll=True)

    chip = me // 2
    middle = (chip == 1) | (chip == 2)
    lead, behind = middle & (me % 2 == 0), middle & (me % 2 == 1)
    to_last = [chip ^ (LINK[l] // 2) == 3 for l in range(2)]
    barrier = pltpu.get_barrier_semaphore()

    def greet(sem, masks):
        for mask in masks:
            pl.semaphore_signal(sem, inc=1, device_id={"tp": me ^ mask}, device_id_type=MESH)

    def when(p, f, *args):
        @pl.when(p)
        def _():
            f(*args)

    def first_rows(l):
        own(l, turn(l, 0), 0, FEW).start()

    def pieces_after(l, lo):
        own(l, turn(l, 0), lo, PIECE).start()
        for k in (1, 2):
            own(l, turn(l, k)).start()

    when(jnp.logical_not(lead), greet, barrier, (SIB,))
    when(chip != 3, greet, barrier, LINK)
    when(behind, pl.semaphore_wait, barrier, 1)
    when(lead, pl.semaphore_wait, barrier, 2)
    when(jnp.logical_not(middle), pl.semaphore_wait, barrier, 3)
    for l in range(2):
        when(behind & jnp.logical_not(to_last[l]), first_rows, l)
        when(jnp.logical_not(behind | to_last[l]), pieces_after, l, 0)
    when(lead, greet, late, (SIB,))
    when(chip == 3, greet, late, LINK)
    for i in range(2):
        weights[i].start()
    when(lead, pl.semaphore_wait, late, 1)
    when(behind, pl.semaphore_wait, late, 2)
    for l in range(2):
        when(to_last[l], pieces_after, l, 0)
    weights[0].wait()
    for l in range(2):
        when(behind & jnp.logical_not(to_last[l]), pieces_after, l, FEW)
    weights[1].wait()
    weights[2].start()
    take(0)
    take_other(0)
    hand_own().start()

    def at(s, table):
        for k, fs in table.items():

            @pl.when(s == k)
            def _(fs=fs):
                for f, *args in fs:
                    f(*args)

    after_tiles = {p + 1: [(settle, p)] for p in range(7)}
    after_gate = {s: [(take, s + 1)] for s in range(7)}
    after_tile = {s: [(take_other, s + 1)] for s in range(7)}
    ends = {s: [(term(s).start,)] for s in range(STEPS)}
    after_gate[7] = []
    after_gate[0].append((weights[2].wait,))
    after_gate[6].append((pass_on, 0))
    ends[7].append((pass_on, 1))
    for s in range(1, STEPS):
        after_gate[s].append((term(s - 1).wait_send,))

    def step(s, carry):
        drain(lx.at[0], 4)
        gate_up(0, 3)
        at(s, after_tiles)
        gate_up(3, ff // GT)
        at(s, after_gate)
        down(0, d // DT - 1)
        at(s, after_tile)
        down(d // DT - 1, d // DT)
        at(s, ends)
        return carry

    lax.fori_loop(0, STEPS, step, 0)

    drain(sent.at[2], 4)
    drain(rf.at[0], 4)
    back = [pltpu.make_async_copy(fh.at[l], xb.at[rows(2 * l, 2)], lx.at[0]) for l in range(2)]
    for c in back:
        c.start()
    drain(lx.at[0], 4)

    def first(i):
        r = pl.ds(i, 16)
        v = xb[r].astype(F32) + xb[pl.ds(2 * PIECE + i, 16)].astype(F32)
        y[r, cols[0]] = (hold[0, r] + v[:, :half]).astype(BF16)
        y[r, cols[1]] = (hold[1, r] + v[:, half:]).astype(BF16)

    blocks(2 * PIECE // 16, first)
    term(7).wait_recv()
    drain(rf.at[1], 2)

    def add_direct(i):
        r = pl.ds(i, 16)
        for c, l in zip(cols, range(2)):
            mine[r, c] += trecv[1, r, c].astype(F32) + fv[l, r, c].astype(F32)

    blocks(2 * PIECE // 16, add_direct)
    for k, n, sem in RELAYED[1]:
        drain(rf.at[sem], 1)

        def add_relayed(i, k=k):
            r = pl.ds(k * PIECE + i, 16)
            for c, l in zip(cols, range(2)):
                v = mine[r, c] + fv[1 - l, r, c].astype(F32)
                y[pl.ds((2 + k) * PIECE + i, 16), c] = v.astype(BF16)

        blocks(n * PIECE // 16, add_relayed)
    term(7).wait_send()
    drain(sent.at[0], 32)
    drain(sent.at[3], 4)


def solution(mesh):
    def step(x, w_gate, w_up, w_down):
        r, d = x.shape
        ff = w_gate.shape[1]
        hbm = pl.BlockSpec(memory_space=pl.ANY)
        dma = pltpu.SemaphoreType.DMA
        half = d // 2
        y, _, _ = pl.pallas_call(
            body,
            out_shape=(
                pltpu.VMEM((r, d), BF16),
                jax.ShapeDtypeStruct((4, 2, r, d), BF16),
                jax.ShapeDtypeStruct((2, 2 * PIECE, d), BF16),
            ),
            in_specs=[hbm] * 4,
            out_specs=(pl.BlockSpec(memory_space=pltpu.VMEM), hbm, hbm),
            scratch_shapes=[
                pltpu.VMEM((d, ff), BF16),
                pltpu.VMEM((d, ff), BF16),
                pltpu.VMEM((ff, d), BF16),
                pltpu.VMEM((256, d), BF16),
                pltpu.VMEM((256, ff), BF16),
                pltpu.VMEM((128, d), F32),
                pltpu.VMEM((128, d), BF16),
                pltpu.VMEM((2, 128, d), BF16),
                pltpu.VMEM((2, 128, d), BF16),
                pltpu.VMEM((2, 2, 128, half), BF16),
                pltpu.VMEM((2, 256, half), F32),
                pltpu.VMEM((2, 2 * PIECE, d), BF16),
                dma((4,)), dma((4,)), dma((2,)), dma((3,)), dma((2,)), dma((2,)), dma((4,)), dma((1,)), dma((3,)),
                pltpu.SemaphoreType.REGULAR,
            ],
            compiler_params=pltpu.CompilerParams(
                collective_id=0, has_side_effects=True, vmem_limit_bytes=64487424
            ),
            cost_estimate=pl.CostEstimate(
                flops=6 * 8 * r * d * ff, bytes_accessed=6 * d * ff + 4 * r * d, transcendentals=8 * r * ff
            ),
            name="mlp",
        )(x, w_gate, w_up, w_down)
        def put(src, dst, sem):
            c = pltpu.make_async_copy(src, dst, sem.at[0])
            c.start()
            c.wait()

        return y

    return jax.shard_map(
        step,
        mesh=mesh,
        in_specs=(P(("dp", "tp"), None), P(None, "tp"), P(None, "tp"), P("tp", None)),
        out_specs=P(("dp", "tp"), None),
        check_vma=False,
    )
```

```python
import jax
import jax.numpy as jnp
from jax import lax
from jax.experimental import pallas as pl
from jax.experimental.pallas import tpu as pltpu
from jax.sharding import PartitionSpec as P

F32 = jnp.float32
BF16 = jnp.bfloat16
MESH = pl.DeviceIdType.MESH

SIB, YN, XN = 1, 2, 4
LINK = (XN, YN)
OWN, FX, FY, DG = 0, 1, 2, 3
PIECE = 64
FEW = 16
STEPS = 8
X_STEPS = {0: 0, 1: 1, 2: 2, 4: 3}
D_STEPS = {3: 0, 5: 1}
SWAP = (1, 0, 3, 2)
GT = 256
DT = 1024


def body(
    x, wg_h, wu_h, wd_h, y, xg, fh,
    wg, wu, wd, xb, hb, mine, tsend, trecv, outg, rly, hold, fv,
    sent, ro, rr, rs, rt, rg, rf, lx, lw, late,
):
    me = lax.axis_index("tp")
    d = x.shape[1]
    half = d // 2
    ff = wg.shape[1]
    cols = (pl.ds(0, half), pl.ds(half, half))

    def remote(src, dst, send, recv, mask):
        return pltpu.make_async_remote_copy(
            src_ref=src, dst_ref=dst, send_sem=send, recv_sem=recv,
            device_id={"tp": me ^ mask}, device_id_type=MESH,
        )

    def rows(k, n=1):
        return pl.ds(k * PIECE, n * PIECE)

    def drain(sem, n):
        ref = {1: xg.at[0, 0, rows(0)], 2: xg.at[0, 0, rows(0, 2)], 4: xg.at[0, 0], 32: xg}[n]
        pltpu.make_async_copy(ref, ref, sem).wait()

    def turn(l, k):
        return SWAP[k] if l else k

    def own(l, k, lo=0, hi=PIECE):
        r = pl.ds(k * PIECE + lo, hi - lo)
        return remote(x.at[r], xg.at[FX + l, 0, r], sent.at[0], ro.at[turn(l, k)], LINK[l])

    def relay(l, r):
        k = 2 * r + 1 - l
        return remote(
            xg.at[FY - l, 0, rows(k)], xg.at[DG, 0, rows(k)], sent.at[0], rr.at[r], LINK[l]
        )

    def hand_own():
        return remote(x, xg.at[OWN, 1], sent.at[0], rs.at[2], SIB)

    def hand(s):
        return [
            remote(xg.at[b, 0, rows(k)], xg.at[b, 1, rows(k)], sent.at[0], rs.at[s % 2], SIB)
            for b, k in pieces(s)
        ]

    def term(s):
        return remote(tsend, trecv.at[s % 2], sent.at[1], rt.at[s % 2], SIB)

    def landing(c):
        return fv if c else fh

    def direct(l, c):
        src = y.at[rows(2 * c, 2), cols[l]]
        return remote(src, landing(c).at[l, :, cols[l]], sent.at[2], rf.at[c], LINK[l])

    def diag(l, c):
        return remote(outg.at[c, :, cols[l]], rly.at[c, l], sent.at[0], rg.at[c], LINK[l])

    def relayed(l, c, k, n, sem):
        dst = landing(c).at[l, rows(k, n), cols[1 - l]]
        return remote(rly.at[c, 1 - l, rows(k, n)], dst, sent.at[3], rf.at[sem], LINK[l])

    RELAYED = (((0, 2, 0),), ((0, 1, 2), (1, 1, 3)))

    def pieces(s):
        if s in X_STEPS:
            return tuple((FX + l, turn(l, X_STEPS[s])) for l in range(2))
        b, c = (DG, D_STEPS[s]) if s in D_STEPS else (OWN, s - 6)
        return ((b, 2 * c), (b, 2 * c + 1))

    def load(s, side):
        out = []
        for i, (b, k) in enumerate(pieces(s)):
            src = x.at[rows(k)] if (b == OWN and side == 0) else xg.at[b, side, rows(k)]
            out.append(pltpu.make_async_copy(src, xb.at[rows(2 * side + i)], lx.at[0]))
        return out

    def take(s):
        if s in X_STEPS:
            drain(ro.at[X_STEPS[s]], 2)
        elif s in D_STEPS:
            drain(rr.at[D_STEPS[s]], 2)
        if s < 6:
            for c in hand(s):
                c.start()
        for c in load(s, 0):
            c.start()
        if s == 1:
            for l in range(2):
                relay(l, 0).start()
                own(l, turn(l, 3)).start()
        if s == 2:
            for l in range(2):
                relay(l, 1).start()

    def take_other(s):
        if s < 6:
            drain(rs.at[s % 2], 2)
        elif s == 6:
            hand_own().wait_recv()
        for c in load(s, 1):
            c.start()

    weights = [
        pltpu.make_async_copy(h, v, lw.at[i])
        for i, (h, v) in enumerate(((wg_h, wg), (wu_h, wu), (wd_h, wd)))
    ]

    def total(r, slot):
        return mine[r] + trecv[slot, r].astype(F32)

    def blocks(n, f):
        def one(i, carry):
            f(pl.multiple_of(i * 16, 16))
            return carry

        lax.fori_loop(0, n, one, 0)

    def settle(p):
        slot = p % 2
        term(p).wait_recv()
        if p in X_STEPS:
            n = X_STEPS[p]
            for l in range(2):

                def f(i, l=l):
                    v = total(pl.ds(l * PIECE + i, 16), slot)
                    a, b = v[:, :half], v[:, half:]
                    r = pl.ds(turn(l, n) * PIECE + i, 16)
                    y[r, cols[l]] = (b if l else a).astype(BF16)
                    hold[l, r] = a if l else b

                blocks(PIECE // 16, f)
            if n % 2:
                for l in range(2):
                    direct(l, n // 2).start()
        elif p in D_STEPS:
            n = D_STEPS[p]

            def f(i):
                r = pl.ds(i, 16)
                outg[n, r] = total(r, slot).astype(BF16)

            blocks(8, f)
            for l in range(2):
                diag(l, n).start()
        else:

            def f(i):
                r = pl.ds(i, 16)
                v = total(r, slot)
                hold[0, r] = v[:, :half]
                hold[1, r] = v[:, half:]

            blocks(8, f)

    def pass_on(c):
        drain(rg.at[c], 2)
        for k, n, sem in RELAYED[c]:
            for l in range(2):

                def f(i, k=k, l=l):
                    r = pl.ds(k * PIECE + i, 16)
                    v = hold[l, pl.ds((2 * c + k) * PIECE + i, 16)] + rly[c, 1 - l, r].astype(F32)
                    rly[c, 1 - l, r] = v.astype(BF16)

                blocks(n * PIECE // 16, f)
                relayed(l, c, k, n, sem).start()

    def gate_up(lo, hi):
        def one(j, carry):
            c = pl.ds(pl.multiple_of(j * GT, GT), GT)
            g = jnp.dot(xb[...], wg[:, c], preferred_element_type=F32)
            u = jnp.dot(xb[...], wu[:, c], preferred_element_type=F32)
            hb[:, c] = (jax.nn.silu(g) * u).astype(BF16)
            return carry

        lax.fori_loop(lo, hi, one, 0, unroll=True)

    def down(lo, hi):
        def one(j, carry):
            c = pl.ds(pl.multiple_of(j * DT, DT), DT)
            t = jnp.dot(hb[...], wd[:, c], preferred_element_type=F32)
            mine[:, c] = t[: 2 * PIECE]
            tsend[:, c] = t[2 * PIECE :].astype(BF16)
            return carry

        lax.fori_loop(lo, hi, one, 0, unroll=True)

    chip = me // 2
    middle = (chip == 1) | (chip == 2)
    lead, behind = middle & (me % 2 == 0), middle & (me % 2 == 1)
    last0, last1 = (chip == 3) & (me % 2 == 0), (chip == 3) & (me % 2 == 1)
    slow = (chip == 0) & (me % 2 == 1)
    to_last = [chip ^ (LINK[l] // 2) == 3 for l in range(2)]
    barrier = pltpu.get_barrier_semaphore()

    def greet(sem, masks):
        for mask in masks:
            pl.semaphore_signal(sem, inc=1, device_id={"tp": me ^ mask}, device_id_type=MESH)

    def when(p, f, *args):
        @pl.when(p)
        def _():
            f(*args)

    def first_rows(l):
        own(l, turn(l, 0), 0, FEW).start()

    def pieces_after(l, lo):
        own(l, turn(l, 0), lo, PIECE).start()
        for k in (1, 2):
            own(l, turn(l, k)).start()

    when(jnp.logical_not(lead | last0), greet, barrier, (SIB,))
    when(chip != 3, greet, barrier, LINK)
    when(behind, pl.semaphore_wait, barrier, 1)
    when(lead, pl.semaphore_wait, barrier, 2)
    when(last1, pl.semaphore_wait, barrier, 2)
    when(jnp.logical_not(middle | last1), pl.semaphore_wait, barrier, 3)
    for l in range(2):
        when((behind & jnp.logical_not(to_last[l])) | slow, first_rows, l)
        when(jnp.logical_not(behind | to_last[l] | slow), pieces_after, l, 0)
    when(lead | last0, greet, late, (SIB,))
    when(chip == 3, greet, late, LINK)
    for i in range(2):
        weights[i].start()
    when(lead | last1, pl.semaphore_wait, late, 1)
    when(behind, pl.semaphore_wait, late, 2)
    for l in range(2):
        when(to_last[l], pieces_after, l, 0)
    weights[0].wait()
    for l in range(2):
        when((behind & jnp.logical_not(to_last[l])) | slow, pieces_after, l, FEW)
    weights[1].wait()
    weights[2].start()
    take(0)
    take_other(0)
    hand_own().start()

    def at(s, table):
        for k, fs in table.items():

            @pl.when(s == k)
            def _(fs=fs):
                for f, *args in fs:
                    f(*args)

    after_tiles = {p + 1: [(settle, p)] for p in range(7)}
    after_gate = {s: [(take, s + 1)] for s in range(7)}
    after_tile = {s: [(take_other, s + 1)] for s in range(7)}
    ends = {s: [(term(s).start,)] for s in range(STEPS)}
    after_gate[7] = []
    after_gate[0].append((weights[2].wait,))
    after_gate[6].append((pass_on, 0))
    ends[7].append((pass_on, 1))
    for s in range(1, STEPS):
        after_gate[s].append((term(s - 1).wait_send,))

    def step(s, carry):
        drain(lx.at[0], 4)
        gate_up(0, 3)
        at(s, after_tiles)
        gate_up(3, ff // GT)
        at(s, after_gate)
        down(0, d // DT - 1)
        at(s, after_tile)
        down(d // DT - 1, d // DT)
        at(s, ends)
        return carry

    lax.fori_loop(0, STEPS, step, 0)

    drain(sent.at[2], 4)
    drain(rf.at[0], 4)
    back = [pltpu.make_async_copy(fh.at[l], xb.at[rows(2 * l, 2)], lx.at[0]) for l in range(2)]
    for c in back:
        c.start()
    drain(lx.at[0], 4)

    def first(i):
        r = pl.ds(i, 16)
        v = xb[r].astype(F32) + xb[pl.ds(2 * PIECE + i, 16)].astype(F32)
        y[r, cols[0]] = (hold[0, r] + v[:, :half]).astype(BF16)
        y[r, cols[1]] = (hold[1, r] + v[:, half:]).astype(BF16)

    blocks(2 * PIECE // 16, first)
    term(7).wait_recv()
    drain(rf.at[1], 2)

    def add_direct(i):
        r = pl.ds(i, 16)
        for c, l in zip(cols, range(2)):
            mine[r, c] += trecv[1, r, c].astype(F32) + fv[l, r, c].astype(F32)

    blocks(2 * PIECE // 16, add_direct)
    for k, n, sem in RELAYED[1]:
        drain(rf.at[sem], 1)

        def add_relayed(i, k=k):
            r = pl.ds(k * PIECE + i, 16)
            for c, l in zip(cols, range(2)):
                v = mine[r, c] + fv[1 - l, r, c].astype(F32)
                y[pl.ds((2 + k) * PIECE + i, 16), c] = v.astype(BF16)

        blocks(n * PIECE // 16, add_relayed)
    term(7).wait_send()
    drain(sent.at[0], 32)
    drain(sent.at[3], 4)


def solution(mesh):
    def step(x, w_gate, w_up, w_down):
        r, d = x.shape
        ff = w_gate.shape[1]
        hbm = pl.BlockSpec(memory_space=pl.ANY)
        dma = pltpu.SemaphoreType.DMA
        half = d // 2
        y, _, _ = pl.pallas_call(
            body,
            out_shape=(
                pltpu.VMEM((r, d), BF16),
                jax.ShapeDtypeStruct((4, 2, r, d), BF16),
                jax.ShapeDtypeStruct((2, 2 * PIECE, d), BF16),
            ),
            in_specs=[hbm] * 4,
            out_specs=(pl.BlockSpec(memory_space=pltpu.VMEM), hbm, hbm),
            scratch_shapes=[
                pltpu.VMEM((d, ff), BF16),
                pltpu.VMEM((d, ff), BF16),
                pltpu.VMEM((ff, d), BF16),
                pltpu.VMEM((256, d), BF16),
                pltpu.VMEM((256, ff), BF16),
                pltpu.VMEM((128, d), F32),
                pltpu.VMEM((128, d), BF16),
                pltpu.VMEM((2, 128, d), BF16),
                pltpu.VMEM((2, 128, d), BF16),
                pltpu.VMEM((2, 2, 128, half), BF16),
                pltpu.VMEM((2, 256, half), F32),
                pltpu.VMEM((2, 2 * PIECE, d), BF16),
                dma((4,)), dma((4,)), dma((2,)), dma((3,)), dma((2,)), dma((2,)), dma((4,)), dma((1,)), dma((3,)),
                pltpu.SemaphoreType.REGULAR,
            ],
            compiler_params=pltpu.CompilerParams(
                collective_id=0, has_side_effects=True, vmem_limit_bytes=64487424
            ),
            cost_estimate=pl.CostEstimate(
                flops=6 * 8 * r * d * ff, bytes_accessed=6 * d * ff + 4 * r * d, transcendentals=8 * r * ff
            ),
            name="mlp",
        )(x, w_gate, w_up, w_down)
        def put(src, dst, sem):
            c = pltpu.make_async_copy(src, dst, sem.at[0])
            c.start()
            c.wait()

        return y

    return jax.shard_map(
        step,
        mesh=mesh,
        in_specs=(P(("dp", "tp"), None), P(None, "tp"), P(None, "tp"), P("tp", None)),
        out_specs=P(("dp", "tp"), None),
        check_vma=False,
    )
```

```python
import jax
import jax.numpy as jnp
from jax import lax
from jax.experimental import pallas as pl
from jax.experimental.pallas import tpu as pltpu
from jax.sharding import PartitionSpec as P

F32 = jnp.float32
BF16 = jnp.bfloat16
MESH = pl.DeviceIdType.MESH

SIB, YN, XN = 1, 2, 4
LINK = (XN, YN)
OWN, FX, FY, DG = 0, 1, 2, 3
PIECE = 64
FEW = 16
STEPS = 8
X_STEPS = {0: 0, 1: 1, 2: 2, 4: 3}
D_STEPS = {3: 0, 5: 1}
SWAP = (1, 0, 3, 2)
GT = 256
DT = 1024


def body(
    x, wg_h, wu_h, wd_h, y, xg, fh,
    wg, wu, wd, xb, hb, mine, tsend, trecv, outg, rly, hold, fv,
    sent, ro, rr, rs, rt, rf, lx, lw, late,
):
    me = lax.axis_index("tp")
    d = x.shape[1]
    half = d // 2
    ff = wg.shape[1]
    cols = (pl.ds(0, half), pl.ds(half, half))

    def remote(src, dst, send, recv, mask):
        return pltpu.make_async_remote_copy(
            src_ref=src, dst_ref=dst, send_sem=send, recv_sem=recv,
            device_id={"tp": me ^ mask}, device_id_type=MESH,
        )

    def rows(k, n=1):
        return pl.ds(k * PIECE, n * PIECE)

    def drain(sem, n):
        ref = {1: xg.at[0, 0, rows(0)], 2: xg.at[0, 0, rows(0, 2)], 4: xg.at[0, 0], 32: xg}[n]
        pltpu.make_async_copy(ref, ref, sem).wait()

    last_sem = (rf.at[0], ro.at[2], ro.at[3], rr.at[0])

    def turn(l, k):
        return SWAP[k] if l else k

    def own(l, k, lo=0, hi=PIECE):
        r = pl.ds(k * PIECE + lo, hi - lo)
        return remote(x.at[r], xg.at[FX + l, 0, r], sent.at[0], ro.at[turn(l, k)], LINK[l])

    def relay(l, r):
        k = 2 * r + 1 - l
        return remote(
            xg.at[FY - l, 0, rows(k)], xg.at[DG, 0, rows(k)], sent.at[0], rr.at[r], LINK[l]
        )

    def hand_own():
        return remote(x, xg.at[OWN, 1], sent.at[0], rs.at[2], SIB)

    def hand(s):
        return [
            remote(xg.at[b, 0, rows(k)], xg.at[b, 1, rows(k)], sent.at[0], rs.at[s % 2], SIB)
            for b, k in pieces(s)
        ]

    def term(s):
        return remote(tsend, trecv.at[s % 2], sent.at[1], rt.at[s % 2], SIB)

    def landing(c):
        return fv if c else fh

    def direct(l, c):
        src = y.at[rows(2 * c, 2), cols[l]]
        return remote(src, landing(c).at[l, :, cols[l]], sent.at[2], last_sem[c], LINK[l])

    def diag(l, c):
        return remote(outg.at[c, :, cols[l]], rly.at[c, l], sent.at[0], ro.at[c], LINK[l])

    def relayed(l, c, k, n, sem):
        dst = landing(c).at[l, rows(k, n), cols[1 - l]]
        return remote(rly.at[c, 1 - l, rows(k, n)], dst, sent.at[3], last_sem[sem], LINK[l])

    RELAYED = (((0, 2, 0),), ((0, 1, 2), (1, 1, 3)))

    def pieces(s):
        if s in X_STEPS:
            return tuple((FX + l, turn(l, X_STEPS[s])) for l in range(2))
        b, c = (DG, D_STEPS[s]) if s in D_STEPS else (OWN, s - 6)
        return ((b, 2 * c), (b, 2 * c + 1))

    def load(s, side):
        out = []
        for i, (b, k) in enumerate(pieces(s)):
            src = x.at[rows(k)] if (b == OWN and side == 0) else xg.at[b, side, rows(k)]
            out.append(pltpu.make_async_copy(src, xb.at[rows(2 * side + i)], lx.at[0]))
        return out

    def take(s):
        if s in X_STEPS:
            drain(ro.at[X_STEPS[s]], 2)
        elif s in D_STEPS:
            drain(rr.at[D_STEPS[s]], 2)
        if s < 6:
            for c in hand(s):
                c.start()
        for c in load(s, 0):
            c.start()
        if s == 1:
            for l in range(2):
                relay(l, 0).start()
                own(l, turn(l, 3)).start()
        if s == 2:
            for l in range(2):
                relay(l, 1).start()

    def take_other(s):
        if s < 6:
            drain(rs.at[s % 2], 2)
        elif s == 6:
            hand_own().wait_recv()
        for c in load(s, 1):
            c.start()

    weights = [
        pltpu.make_async_copy(h, v, lw.at[0] if i else lx.at[0])
        for i, (h, v) in enumerate(((wg_h, wg), (wu_h, wu), (wd_h, wd)))
    ]

    def total(r, slot):
        return mine[r] + trecv[slot, r].astype(F32)

    def blocks(n, f):
        def one(i, carry):
            f(pl.multiple_of(i * 16, 16))
            return carry

        lax.fori_loop(0, n, one, 0)

    def settle(p):
        slot = p % 2
        term(p).wait_recv()
        if p in X_STEPS:
            n = X_STEPS[p]
            for l in range(2):

                def f(i, l=l):
                    v = total(pl.ds(l * PIECE + i, 16), slot)
                    a, b = v[:, :half], v[:, half:]
                    r = pl.ds(turn(l, n) * PIECE + i, 16)
                    y[r, cols[l]] = (b if l else a).astype(BF16)
                    hold[l, r] = a if l else b

                blocks(PIECE // 16, f)
            if n % 2:
                for l in range(2):
                    direct(l, n // 2).start()
        elif p in D_STEPS:
            n = D_STEPS[p]

            def f(i):
                r = pl.ds(i, 16)
                outg[n, r] = total(r, slot).astype(BF16)

            blocks(8, f)
            for l in range(2):
                diag(l, n).start()
        else:

            def f(i):
                r = pl.ds(i, 16)
                v = total(r, slot)
                hold[0, r] = v[:, :half]
                hold[1, r] = v[:, half:]

            blocks(8, f)

    def pass_on(c):
        drain(ro.at[c], 2)
        for k, n, sem in RELAYED[c]:
            for l in range(2):

                def f(i, k=k, l=l):
                    r = pl.ds(k * PIECE + i, 16)
                    v = hold[l, pl.ds((2 * c + k) * PIECE + i, 16)] + rly[c, 1 - l, r].astype(F32)
                    rly[c, 1 - l, r] = v.astype(BF16)

                blocks(n * PIECE // 16, f)
                relayed(l, c, k, n, sem).start()

    def gate_up(lo, hi):
        def one(j, carry):
            c = pl.ds(pl.multiple_of(j * GT, GT), GT)
            g = jnp.dot(xb[...], wg[:, c], preferred_element_type=F32)
            u = jnp.dot(xb[...], wu[:, c], preferred_element_type=F32)
            hb[:, c] = (jax.nn.silu(g) * u).astype(BF16)
            return carry

        lax.fori_loop(lo, hi, one, 0, unroll=True)

    def down(lo, hi):
        def one(j, carry):
            c = pl.ds(pl.multiple_of(j * DT, DT), DT)
            t = jnp.dot(hb[...], wd[:, c], preferred_element_type=F32)
            mine[:, c] = t[: 2 * PIECE]
            tsend[:, c] = t[2 * PIECE :].astype(BF16)
            return carry

        lax.fori_loop(lo, hi, one, 0, unroll=True)

    chip = me // 2
    middle = (chip == 1) | (chip == 2)
    lead, behind = middle & (me % 2 == 0), middle & (me % 2 == 1)
    last0, last1 = (chip == 3) & (me % 2 == 0), (chip == 3) & (me % 2 == 1)
    slow = (chip == 0) & (me % 2 == 1)
    to_last = [chip ^ (LINK[l] // 2) == 3 for l in range(2)]
    barrier = pltpu.get_barrier_semaphore()

    def greet(sem, masks):
        for mask in masks:
            pl.semaphore_signal(sem, inc=1, device_id={"tp": me ^ mask}, device_id_type=MESH)

    def when(p, f, *args):
        @pl.when(p)
        def _():
            f(*args)

    def first_rows(l):
        own(l, turn(l, 0), 0, FEW).start()

    def pieces_after(l, lo):
        own(l, turn(l, 0), lo, PIECE).start()
        for k in (1, 2):
            own(l, turn(l, k)).start()

    when(jnp.logical_not(lead | last0), greet, barrier, (SIB,))
    when(chip != 3, greet, barrier, LINK)
    when(behind, pl.semaphore_wait, barrier, 1)
    when(lead, pl.semaphore_wait, barrier, 2)
    when(last1, pl.semaphore_wait, barrier, 2)
    when(jnp.logical_not(middle | last1), pl.semaphore_wait, barrier, 3)
    for l in range(2):
        when((behind & jnp.logical_not(to_last[l])) | slow, first_rows, l)
        when(jnp.logical_not(behind | to_last[l] | slow), pieces_after, l, 0)
    when(lead | last0, greet, late, (SIB,))
    when(chip == 3, greet, late, LINK)
    for i in range(2):
        weights[i].start()
    when(lead | last1, pl.semaphore_wait, late, 1)
    when(behind, pl.semaphore_wait, late, 2)
    for l in range(2):
        when(to_last[l], pieces_after, l, 0)
    weights[0].wait()
    for l in range(2):
        when((behind & jnp.logical_not(to_last[l])) | slow, pieces_after, l, FEW)
    weights[1].wait()
    weights[2].start()
    take(0)
    take_other(0)
    hand_own().start()

    def at(s, table):
        for k, fs in table.items():

            @pl.when(s == k)
            def _(fs=fs):
                for f, *args in fs:
                    f(*args)

    after_tiles = {p + 1: [(settle, p)] for p in range(7)}
    after_gate = {s: [(take, s + 1)] for s in range(7)}
    after_tile = {s: [(take_other, s + 1)] for s in range(7)}
    ends = {s: [(term(s).start,)] for s in range(STEPS)}
    after_gate[7] = []
    after_gate[0].append((weights[2].wait,))
    after_gate[6].append((pass_on, 0))
    ends[7].append((pass_on, 1))
    for s in range(1, STEPS):
        after_gate[s].append((term(s - 1).wait_send,))

    def step(s, carry):
        drain(lx.at[0], 4)
        gate_up(0, 3)
        at(s, after_tiles)
        gate_up(3, ff // GT)
        at(s, after_gate)
        down(0, d // DT - 1)
        at(s, after_tile)
        down(d // DT - 1, d // DT)
        at(s, ends)
        return carry

    lax.fori_loop(0, STEPS, step, 0)

    drain(sent.at[2], 4)
    drain(rf.at[0], 4)
    back = [pltpu.make_async_copy(fh.at[l], xb.at[rows(2 * l, 2)], lx.at[0]) for l in range(2)]
    for c in back:
        c.start()
    drain(lx.at[0], 4)

    def first(i):
        r = pl.ds(i, 16)
        v = xb[r].astype(F32) + xb[pl.ds(2 * PIECE + i, 16)].astype(F32)
        y[r, cols[0]] = (hold[0, r] + v[:, :half]).astype(BF16)
        y[r, cols[1]] = (hold[1, r] + v[:, half:]).astype(BF16)

    blocks(2 * PIECE // 16, first)
    term(7).wait_recv()
    drain(last_sem[1], 2)

    def add_direct(i):
        r = pl.ds(i, 16)
        for c, l in zip(cols, range(2)):
            mine[r, c] += trecv[1, r, c].astype(F32) + fv[l, r, c].astype(F32)

    blocks(2 * PIECE // 16, add_direct)
    for k, n, sem in RELAYED[1]:
        drain(last_sem[sem], 1)

        def add_relayed(i, k=k):
            r = pl.ds(k * PIECE + i, 16)
            for c, l in zip(cols, range(2)):
                v = mine[r, c] + fv[1 - l, r, c].astype(F32)
                y[pl.ds((2 + k) * PIECE + i, 16), c] = v.astype(BF16)

        blocks(n * PIECE // 16, add_relayed)
    term(7).wait_send()
    drain(sent.at[0], 32)
    drain(sent.at[3], 4)


def solution(mesh):
    def step(x, w_gate, w_up, w_down):
        r, d = x.shape
        ff = w_gate.shape[1]
        hbm = pl.BlockSpec(memory_space=pl.ANY)
        dma = pltpu.SemaphoreType.DMA
        half = d // 2
        y, _, _ = pl.pallas_call(
            body,
            out_shape=(
                pltpu.VMEM((r, d), BF16),
                jax.ShapeDtypeStruct((4, 2, r, d), BF16),
                jax.ShapeDtypeStruct((2, 2 * PIECE, d), BF16),
            ),
            in_specs=[hbm] * 4,
            out_specs=(pl.BlockSpec(memory_space=pltpu.VMEM), hbm, hbm),
            scratch_shapes=[
                pltpu.VMEM((d, ff), BF16),
                pltpu.VMEM((d, ff), BF16),
                pltpu.VMEM((ff, d), BF16),
                pltpu.VMEM((256, d), BF16),
                pltpu.VMEM((256, ff), BF16),
                pltpu.VMEM((128, d), F32),
                pltpu.VMEM((128, d), BF16),
                pltpu.VMEM((2, 128, d), BF16),
                pltpu.VMEM((2, 128, d), BF16),
                pltpu.VMEM((2, 2, 128, half), BF16),
                pltpu.VMEM((2, 256, half), F32),
                pltpu.VMEM((2, 2 * PIECE, d), BF16),
                dma((4,)), dma((4,)), dma((2,)), dma((3,)), dma((2,)), dma((1,)), dma((1,)), dma((1,)),
                pltpu.SemaphoreType.REGULAR,
            ],
            compiler_params=pltpu.CompilerParams(
                collective_id=0, has_side_effects=True, vmem_limit_bytes=64487424
            ),
            cost_estimate=pl.CostEstimate(
                flops=6 * 8 * r * d * ff, bytes_accessed=6 * d * ff + 4 * r * d, transcendentals=8 * r * ff
            ),
            name="mlp",
        )(x, w_gate, w_up, w_down)
        def put(src, dst, sem):
            c = pltpu.make_async_copy(src, dst, sem.at[0])
            c.start()
            c.wait()

        return y

    return jax.shard_map(
        step,
        mesh=mesh,
        in_specs=(P(("dp", "tp"), None), P(None, "tp"), P(None, "tp"), P("tp", None)),
        out_specs=P(("dp", "tp"), None),
        check_vma=False,
    )
```

```python
import jax
import jax.numpy as jnp
from jax import lax
from jax.experimental import pallas as pl
from jax.experimental.pallas import tpu as pltpu
from jax.sharding import PartitionSpec as P

F32 = jnp.float32
BF16 = jnp.bfloat16
MESH = pl.DeviceIdType.MESH

SIB, YN, XN = 1, 2, 4
LINK = (XN, YN)
OWN, FX, FY, DG = 0, 1, 2, 3
PIECE = 64
FEW = 16
STEPS = 8
X_STEPS = {0: 0, 1: 1, 2: 2, 4: 3}
D_STEPS = {3: 0, 5: 1}
SWAP = (1, 0, 3, 2)
GT = 256
DT = 1024


def body(
    x, wg_h, wu_h, wd_h, y, xg, fh,
    wg, wu, wd, xb, hb, mine, tsend, trecv, outg, rly, hold, fv,
    sent, ro, rr, rs, rt, rf, lx, late,
):
    me = lax.axis_index("tp")
    d = x.shape[1]
    half = d // 2
    ff = wg.shape[1]
    cols = (pl.ds(0, half), pl.ds(half, half))

    def remote(src, dst, send, recv, mask):
        return pltpu.make_async_remote_copy(
            src_ref=src, dst_ref=dst, send_sem=send, recv_sem=recv,
            device_id={"tp": me ^ mask}, device_id_type=MESH,
        )

    def rows(k, n=1):
        return pl.ds(k * PIECE, n * PIECE)

    def drain(sem, n):
        ref = {1: xg.at[0, 0, rows(0)], 2: xg.at[0, 0, rows(0, 2)], 4: xg.at[0, 0], 32: xg}[n]
        pltpu.make_async_copy(ref, ref, sem).wait()

    last_sem = (rf.at[0], ro.at[2], ro.at[3], rr.at[0])

    def turn(l, k):
        return SWAP[k] if l else k

    def own(l, k, lo=0, hi=PIECE):
        r = pl.ds(k * PIECE + lo, hi - lo)
        return remote(x.at[r], xg.at[FX + l, 0, r], sent.at[0], ro.at[turn(l, k)], LINK[l])

    def relay(l, r):
        k = 2 * r + 1 - l
        return remote(
            xg.at[FY - l, 0, rows(k)], xg.at[DG, 0, rows(k)], sent.at[0], rr.at[r], LINK[l]
        )

    def hand_own():
        return remote(x, xg.at[OWN, 1], sent.at[0], rs.at[2], SIB)

    def hand(s):
        return [
            remote(xg.at[b, 0, rows(k)], xg.at[b, 1, rows(k)], sent.at[0], rs.at[s % 2], SIB)
            for b, k in pieces(s)
        ]

    def term(s):
        return remote(tsend, trecv.at[s % 2], sent.at[1], rt.at[s % 2], SIB)

    def landing(c):
        return fv if c else fh

    def direct(l, c):
        src = y.at[rows(2 * c, 2), cols[l]]
        return remote(src, landing(c).at[l, :, cols[l]], sent.at[2], last_sem[c], LINK[l])

    def diag(l, c):
        return remote(outg.at[c, :, cols[l]], rly.at[c, l], sent.at[0], ro.at[c], LINK[l])

    def relayed(l, c, k, n, sem):
        dst = landing(c).at[l, rows(k, n), cols[1 - l]]
        return remote(rly.at[c, 1 - l, rows(k, n)], dst, sent.at[3], last_sem[sem], LINK[l])

    RELAYED = (((0, 2, 0),), ((0, 1, 2), (1, 1, 3)))

    def pieces(s):
        if s in X_STEPS:
            return tuple((FX + l, turn(l, X_STEPS[s])) for l in range(2))
        b, c = (DG, D_STEPS[s]) if s in D_STEPS else (OWN, s - 6)
        return ((b, 2 * c), (b, 2 * c + 1))

    def load(s, side):
        out = []
        for i, (b, k) in enumerate(pieces(s)):
            src = x.at[rows(k)] if (b == OWN and side == 0) else xg.at[b, side, rows(k)]
            out.append(pltpu.make_async_copy(src, xb.at[rows(2 * side + i)], lx.at[0]))
        return out

    def take(s):
        if s in X_STEPS:
            drain(ro.at[X_STEPS[s]], 2)
        elif s in D_STEPS:
            drain(rr.at[D_STEPS[s]], 2)
        if s < 6:
            for c in hand(s):
                c.start()
        for c in load(s, 0):
            c.start()
        if s == 1:
            for l in range(2):
                relay(l, 0).start()
                own(l, turn(l, 3)).start()
        if s == 2:
            for l in range(2):
                relay(l, 1).start()

    def take_other(s):
        if s < 6:
            drain(rs.at[s % 2], 2)
        elif s == 6:
            hand_own().wait_recv()
        for c in load(s, 1):
            c.start()

    weights = [
        pltpu.make_async_copy(h, v, (lx.at[0], rt.at[0], rt.at[1])[i])
        for i, (h, v) in enumerate(((wg_h, wg), (wu_h, wu), (wd_h, wd)))
    ]

    def total(r, slot):
        return mine[r] + trecv[slot, r].astype(F32)

    def blocks(n, f):
        def one(i, carry):
            f(pl.multiple_of(i * 16, 16))
            return carry

        lax.fori_loop(0, n, one, 0)

    def settle(p):
        slot = p % 2
        term(p).wait_recv()
        if p in X_STEPS:
            n = X_STEPS[p]
            for l in range(2):

                def f(i, l=l):
                    v = total(pl.ds(l * PIECE + i, 16), slot)
                    a, b = v[:, :half], v[:, half:]
                    r = pl.ds(turn(l, n) * PIECE + i, 16)
                    y[r, cols[l]] = (b if l else a).astype(BF16)
                    hold[l, r] = a if l else b

                blocks(PIECE // 16, f)
            if n % 2:
                for l in range(2):
                    direct(l, n // 2).start()
        elif p in D_STEPS:
            n = D_STEPS[p]

            def f(i):
                r = pl.ds(i, 16)
                outg[n, r] = total(r, slot).astype(BF16)

            blocks(8, f)
            for l in range(2):
                diag(l, n).start()
        else:

            def f(i):
                r = pl.ds(i, 16)
                v = total(r, slot)
                hold[0, r] = v[:, :half]
                hold[1, r] = v[:, half:]

            blocks(8, f)

    def pass_on(c):
        drain(ro.at[c], 2)
        for k, n, sem in RELAYED[c]:
            for l in range(2):

                def f(i, k=k, l=l):
                    r = pl.ds(k * PIECE + i, 16)
                    v = hold[l, pl.ds((2 * c + k) * PIECE + i, 16)] + rly[c, 1 - l, r].astype(F32)
                    rly[c, 1 - l, r] = v.astype(BF16)

                blocks(n * PIECE // 16, f)
                relayed(l, c, k, n, sem).start()

    def gate_up(lo, hi):
        def one(j, carry):
            c = pl.ds(pl.multiple_of(j * GT, GT), GT)
            g = jnp.dot(xb[...], wg[:, c], preferred_element_type=F32)
            u = jnp.dot(xb[...], wu[:, c], preferred_element_type=F32)
            hb[:, c] = (jax.nn.silu(g) * u).astype(BF16)
            return carry

        lax.fori_loop(lo, hi, one, 0, unroll=True)

    def down(lo, hi):
        def one(j, carry):
            c = pl.ds(pl.multiple_of(j * DT, DT), DT)
            t = jnp.dot(hb[...], wd[:, c], preferred_element_type=F32)
            mine[:, c] = t[: 2 * PIECE]
            tsend[:, c] = t[2 * PIECE :].astype(BF16)
            return carry

        lax.fori_loop(lo, hi, one, 0, unroll=True)

    chip = me // 2
    middle = (chip == 1) | (chip == 2)
    lead, behind = middle & (me % 2 == 0), middle & (me % 2 == 1)
    last0, last1 = (chip == 3) & (me % 2 == 0), (chip == 3) & (me % 2 == 1)
    slow = (chip == 0) & (me % 2 == 1)
    to_last = [chip ^ (LINK[l] // 2) == 3 for l in range(2)]
    barrier = pltpu.get_barrier_semaphore()

    def greet(sem, masks):
        for mask in masks:
            pl.semaphore_signal(sem, inc=1, device_id={"tp": me ^ mask}, device_id_type=MESH)

    def when(p, f, *args):
        @pl.when(p)
        def _():
            f(*args)

    def first_rows(l):
        own(l, turn(l, 0), 0, FEW).start()

    def pieces_after(l, lo):
        own(l, turn(l, 0), lo, PIECE).start()
        for k in (1, 2):
            own(l, turn(l, k)).start()

    when(jnp.logical_not(lead | last0), greet, barrier, (SIB,))
    when(chip != 3, greet, barrier, LINK)
    when(behind, pl.semaphore_wait, barrier, 1)
    when(lead, pl.semaphore_wait, barrier, 2)
    when(last1, pl.semaphore_wait, barrier, 2)
    when(jnp.logical_not(middle | last1), pl.semaphore_wait, barrier, 3)
    for l in range(2):
        when((behind & jnp.logical_not(to_last[l])) | slow, first_rows, l)
        when(jnp.logical_not(behind | to_last[l] | slow), pieces_after, l, 0)
    when(lead | last0, greet, late, (SIB,))
    when(chip == 3, greet, late, LINK)
    for i in range(2):
        weights[i].start()
    when(lead | last1, pl.semaphore_wait, late, 1)
    when(behind, pl.semaphore_wait, late, 2)
    for l in range(2):
        when(to_last[l], pieces_after, l, 0)
    weights[0].wait()
    for l in range(2):
        when((behind & jnp.logical_not(to_last[l])) | slow, pieces_after, l, FEW)
    weights[1].wait()
    weights[2].start()
    take(0)
    take_other(0)
    hand_own().start()

    def at(s, table):
        for k, fs in table.items():

            @pl.when(s == k)
            def _(fs=fs):
                for f, *args in fs:
                    f(*args)

    after_tiles = {p + 1: [(settle, p)] for p in range(7)}
    after_gate = {s: [(take, s + 1)] for s in range(7)}
    after_tile = {s: [(take_other, s + 1)] for s in range(7)}
    ends = {s: [(term(s).start,)] for s in range(STEPS)}
    after_gate[7] = []
    after_gate[0].append((weights[2].wait,))
    after_gate[6].append((pass_on, 0))
    ends[7].append((pass_on, 1))
    for s in range(1, STEPS):
        after_gate[s].append((term(s - 1).wait_send,))

    def step(s, carry):
        drain(lx.at[0], 4)
        gate_up(0, 3)
        at(s, after_tiles)
        gate_up(3, ff // GT)
        at(s, after_gate)
        down(0, d // DT - 1)
        at(s, after_tile)
        down(d // DT - 1, d // DT)
        at(s, ends)
        return carry

    lax.fori_loop(0, STEPS, step, 0)

    drain(sent.at[2], 4)
    drain(rf.at[0], 4)
    back = [pltpu.make_async_copy(fh.at[l], xb.at[rows(2 * l, 2)], lx.at[0]) for l in range(2)]
    for c in back:
        c.start()
    drain(lx.at[0], 4)

    def first(i):
        r = pl.ds(i, 16)
        v = xb[r].astype(F32) + xb[pl.ds(2 * PIECE + i, 16)].astype(F32)
        y[r, cols[0]] = (hold[0, r] + v[:, :half]).astype(BF16)
        y[r, cols[1]] = (hold[1, r] + v[:, half:]).astype(BF16)

    blocks(2 * PIECE // 16, first)
    term(7).wait_recv()
    drain(last_sem[1], 2)

    def add_direct(i):
        r = pl.ds(i, 16)
        for c, l in zip(cols, range(2)):
            mine[r, c] += trecv[1, r, c].astype(F32) + fv[l, r, c].astype(F32)

    blocks(2 * PIECE // 16, add_direct)
    for k, n, sem in RELAYED[1]:
        drain(last_sem[sem], 1)

        def add_relayed(i, k=k):
            r = pl.ds(k * PIECE + i, 16)
            for c, l in zip(cols, range(2)):
                v = mine[r, c] + fv[1 - l, r, c].astype(F32)
                y[pl.ds((2 + k) * PIECE + i, 16), c] = v.astype(BF16)

        blocks(n * PIECE // 16, add_relayed)
    term(7).wait_send()
    drain(sent.at[0], 32)
    drain(sent.at[3], 4)


def solution(mesh):
    def step(x, w_gate, w_up, w_down):
        r, d = x.shape
        ff = w_gate.shape[1]
        hbm = pl.BlockSpec(memory_space=pl.ANY)
        dma = pltpu.SemaphoreType.DMA
        half = d // 2
        y, _, _ = pl.pallas_call(
            body,
            out_shape=(
                pltpu.VMEM((r, d), BF16),
                jax.ShapeDtypeStruct((4, 2, r, d), BF16),
                jax.ShapeDtypeStruct((2, 2 * PIECE, d), BF16),
            ),
            in_specs=[hbm] * 4,
            out_specs=(pl.BlockSpec(memory_space=pltpu.VMEM), hbm, hbm),
            scratch_shapes=[
                pltpu.VMEM((d, ff), BF16),
                pltpu.VMEM((d, ff), BF16),
                pltpu.VMEM((ff, d), BF16),
                pltpu.VMEM((256, d), BF16),
                pltpu.VMEM((256, ff), BF16),
                pltpu.VMEM((128, d), F32),
                pltpu.VMEM((128, d), BF16),
                pltpu.VMEM((2, 128, d), BF16),
                pltpu.VMEM((2, 128, d), BF16),
                pltpu.VMEM((2, 2, 128, half), BF16),
                pltpu.VMEM((2, 256, half), F32),
                pltpu.VMEM((2, 2 * PIECE, d), BF16),
                dma((4,)), dma((4,)), dma((2,)), dma((3,)), dma((2,)), dma((1,)), dma((1,)),
                pltpu.SemaphoreType.REGULAR,
            ],
            compiler_params=pltpu.CompilerParams(
                collective_id=0, has_side_effects=True, vmem_limit_bytes=64487424
            ),
            cost_estimate=pl.CostEstimate(
                flops=6 * 8 * r * d * ff, bytes_accessed=6 * d * ff + 4 * r * d, transcendentals=8 * r * ff
            ),
            name="mlp",
        )(x, w_gate, w_up, w_down)
        def put(src, dst, sem):
            c = pltpu.make_async_copy(src, dst, sem.at[0])
            c.start()
            c.wait()

        return y

    return jax.shard_map(
        step,
        mesh=mesh,
        in_specs=(P(("dp", "tp"), None), P(None, "tp"), P(None, "tp"), P("tp", None)),
        out_specs=P(("dp", "tp"), None),
        check_vma=False,
    )
```
